32 devices in a mesh: videos: 1 (over z), tokens: 4 (over y), frames: 8 (over x, core).
Axes of the slice: x: 4, y: 4, z: 1, core: 2. Of those that a mesh axis runs over, the one named last changes fastest.
The devices are a block of a 4x4x8 slice.
Arguments:
- z_queue: float32 [128, 256, 4], P(('videos', 'frames'), 'tokens')
- ada_mod: float32 [128, 2, 6, 768], P(('videos', 'frames'))
- step_size: float32 [128], P(('videos', 'frames'))
- new_noise: float32 [6, 256, 4], P('videos', 'tokens')
- lag_bias: float32 [2, 12, 16], replicated
- w_in: bfloat16 [4, 768], replicated
- w_out: bfloat16 [768, 4], replicated
- w_sqkv: bfloat16 [2, 768, 3, 12, 64], replicated
- w_so: bfloat16 [2, 12, 64, 768], replicated
- w_tqkv: bfloat16 [2, 768, 3, 12, 64], replicated
- w_to: bfloat16 [2, 12, 64, 768], replicated
- w_up: bfloat16 [2, 768, 3072], replicated
- w_down: bfloat16 [2, 3072, 768], replicated
Outputs:
- output 1: float32 [6, 256, 4], P('videos', ('tokens', 'frames'))
- output 2: float32 [128, 256, 4], P(('videos', 'frames'), 'tokens')
All inputs are finite; a program needn't handle non-finite values.
Results may differ from the reference program's by a relative error of at most 0.0155034.
Values are sent between devices in bfloat16 or wider.
A program may use at most 768 MiB of HBM per device.

```python
import jax
import jax.numpy as jnp
from jax import lax

FRAMES = 128
PATCHES = 256
CHANNELS = 4
D = 768
HEADS = 12
HEAD = 64
WINDOW = 16
LAYERS = 2
STEPS = 6


def setup_inputs(seed: int = 0, part: int = 0) -> dict:
    base_key = jax.random.key(seed)
    part_keys = jax.random.split(jax.random.fold_in(base_key, part), 4)
    shared_keys = jax.random.split(jax.random.fold_in(base_key, 100003), 9)
    z_queue = jax.random.normal(part_keys[0], (FRAMES, PATCHES, CHANNELS), jnp.float32)
    ada_mod = 0.4 * jax.random.normal(part_keys[1], (FRAMES, LAYERS, 6, D), jnp.float32)
    step_size = jax.random.uniform(part_keys[2], (FRAMES,), jnp.float32, 0.2, 0.6)
    new_noise = jax.random.normal(part_keys[3], (STEPS, PATCHES, CHANNELS), jnp.float32)
    lag_bias = jax.random.normal(shared_keys[0], (LAYERS, HEADS, WINDOW), jnp.float32)
    qkv_gain = jnp.array([2.0, 1.0, 1.0], jnp.float32)[:, None, None]
    w_in = (jax.random.normal(shared_keys[1], (CHANNELS, D), jnp.float32) * CHANNELS ** -0.5).astype(jnp.bfloat16)
    w_out = (jax.random.normal(shared_keys[2], (D, CHANNELS), jnp.float32) * D ** -0.5).astype(jnp.bfloat16)
    w_sqkv = (jax.random.normal(shared_keys[3], (LAYERS, D, 3, HEADS, HEAD), jnp.float32) * qkv_gain * D ** -0.5).astype(jnp.bfloat16)
    w_so = (jax.random.normal(shared_keys[4], (LAYERS, HEADS, HEAD, D), jnp.float32) * D ** -0.5).astype(jnp.bfloat16)
    w_tqkv = (jax.random.normal(shared_keys[5], (LAYERS, D, 3, HEADS, HEAD), jnp.float32) * D ** -0.5).astype(jnp.bfloat16)
    w_to = (jax.random.normal(shared_keys[6], (LAYERS, HEADS, HEAD, D), jnp.float32) * D ** -0.5).astype(jnp.bfloat16)
    w_up = (jax.random.normal(shared_keys[7], (LAYERS, D, 4 * D), jnp.float32) * D ** -0.5).astype(jnp.bfloat16)
    w_down = (jax.random.normal(shared_keys[8], (LAYERS, 4 * D, D), jnp.float32) * (4 * D) ** -0.5).astype(jnp.bfloat16)
    return dict(z_queue=z_queue, ada_mod=ada_mod, step_size=step_size, new_noise=new_noise, lag_bias=lag_bias, w_in=w_in, w_out=w_out, w_sqkv=w_sqkv, w_so=w_so, w_tqkv=w_tqkv, w_to=w_to, w_up=w_up, w_down=w_down)


def layer_norm(xres):
    row_mean = jnp.mean(xres, axis=-1, keepdims=True)
    centered = xres - row_mean
    row_var = jnp.mean(centered * centered, axis=-1, keepdims=True)
    return centered * lax.rsqrt(row_var + 1e-6)


def modulate(xres, mod_l, which):
    shift_vec = mod_l[..., None, 2 * which, :]
    scale_vec = mod_l[..., None, 2 * which + 1, :]
    return (layer_norm(xres) * (1.0 + scale_vec) + shift_vec).astype(jnp.bfloat16)


def spatial_attention(u_act, w_qkv, w_proj):
    qkv_all = jnp.dot(u_act.reshape(-1, D), w_qkv.reshape(D, 3 * D), preferred_element_type=jnp.float32).astype(jnp.bfloat16).reshape(FRAMES, PATCHES, 3, HEADS, HEAD)

    def frame_attention(frame_qkv):
        qkv_wide = frame_qkv.astype(jnp.float32)
        scores = jnp.einsum('qhe,khe->hqk', qkv_wide[:, 0], qkv_wide[:, 1]) * HEAD ** -0.5
        attn_prob = jax.nn.softmax(scores, axis=-1).astype(jnp.bfloat16).astype(jnp.float32)
        return jnp.einsum('hqk,khe->qhe', attn_prob, qkv_wide[:, 2]).astype(jnp.bfloat16)

    attn_out = lax.map(frame_attention, qkv_all)
    return jnp.dot(attn_out.reshape(-1, D), w_proj.reshape(D, D), preferred_element_type=jnp.float32).reshape(FRAMES, PATCHES, D)


def temporal_attention(u_act, w_qkv, w_proj, lag_bias):
    qkv_all = jnp.dot(u_act.reshape(-1, D), w_qkv.reshape(D, 3 * D), preferred_element_type=jnp.float32).astype(jnp.bfloat16).reshape(FRAMES, PATCHES, 3, HEADS, HEAD)
    by_token = jnp.swapaxes(qkv_all, 0, 1)
    offset_idx = jnp.arange(WINDOW)[:, None, None]
    frame_idx = jnp.arange(FRAMES)[None, :, None]
    bias_rows = jnp.transpose(lag_bias)[:, None, :]

    def token_attention(tok_qkv):
        qkv_wide = tok_qkv.astype(jnp.float32)
        keys_pad = jnp.pad(qkv_wide[:, 1], ((WINDOW - 1, 0), (0, 0), (0, 0)))
        vals_pad = jnp.pad(qkv_wide[:, 2], ((WINDOW - 1, 0), (0, 0), (0, 0)))
        scores = jnp.stack([jnp.sum(qkv_wide[:, 0] * keys_pad[WINDOW - 1 - offset:WINDOW - 1 - offset + FRAMES], axis=-1) for offset in range(WINDOW)], axis=0)
        scores = scores * HEAD ** -0.5 + bias_rows
        scores = jnp.where(frame_idx >= offset_idx, scores, -1e30)
        attn_prob = jax.nn.softmax(scores, axis=0).astype(jnp.bfloat16).astype(jnp.float32)
        mixed = sum(attn_prob[offset][:, :, None] * vals_pad[WINDOW - 1 - offset:WINDOW - 1 - offset + FRAMES] for offset in range(WINDOW))
        return mixed.astype(jnp.bfloat16)

    attn_out = jnp.swapaxes(lax.map(token_attention, by_token), 0, 1)
    return jnp.dot(attn_out.reshape(-1, D), w_proj.reshape(D, D), preferred_element_type=jnp.float32).reshape(FRAMES, PATCHES, D)


def mlp_block(u_act, w_up, w_down):
    hidden = jnp.dot(u_act.reshape(-1, D), w_up, preferred_element_type=jnp.float32)
    act_out = jax.nn.gelu(hidden, approximate=True).astype(jnp.bfloat16)
    return jnp.dot(act_out, w_down, preferred_element_type=jnp.float32).reshape(FRAMES, PATCHES, D)


def denoise(z_cur, ada_mod, step_size, lag_bias, w_in, w_out, w_sqkv, w_so, w_tqkv, w_to, w_up, w_down):
    xres = jnp.dot(z_cur.astype(jnp.bfloat16).reshape(-1, CHANNELS), w_in, preferred_element_type=jnp.float32).astype(jnp.bfloat16).astype(jnp.float32).reshape(FRAMES, PATCHES, D)

    def one_layer(xcur, layer_in):
        mod_l, bias_l, sqkv_l, so_l, tqkv_l, to_l, up_l, down_l = layer_in
        xcur = xcur + spatial_attention(modulate(xcur, mod_l, 0), sqkv_l, so_l)
        xcur = xcur + temporal_attention(modulate(xcur, mod_l, 1), tqkv_l, to_l, bias_l)
        xcur = xcur + mlp_block(modulate(xcur, mod_l, 2), up_l, down_l)
        return xcur, None

    xres = lax.scan(one_layer, xres, (jnp.swapaxes(ada_mod, 0, 1), lag_bias, w_sqkv, w_so, w_tqkv, w_to, w_up, w_down))[0]
    velocity = jnp.dot(layer_norm(xres).astype(jnp.bfloat16).reshape(-1, D), w_out, preferred_element_type=jnp.float32).reshape(FRAMES, PATCHES, CHANNELS)
    return z_cur + step_size[:, None, None] * velocity


def reference(z_queue, ada_mod, step_size, new_noise, lag_bias, w_in, w_out, w_sqkv, w_so, w_tqkv, w_to, w_up, w_down):
    def one_step(z_cur, noise_frame):
        z_new = denoise(z_cur, ada_mod, step_size, lag_bias, w_in, w_out, w_sqkv, w_so, w_tqkv, w_to, w_up, w_down)
        return jnp.concatenate([z_new[1:], noise_frame[None]], axis=0), z_new[0]

    z_final, emitted = lax.scan(one_step, z_queue, new_noise)
    return emitted, z_final
```

```python
import functools

import jax
import jax.numpy as jnp
from jax import lax
from jax.experimental import pallas as pl
from jax.experimental.pallas import tpu as pltpu
from jax.sharding import PartitionSpec as P

MESH = pl.DeviceIdType.MESH
BF = jnp.bfloat16
F32 = jnp.float32
LANES = 128
SUB = 8
CHUNKS = 2


def mm(a, b):
    return jnp.dot(a, b, preferred_element_type=F32)


def mm_t(a, b):
    return lax.dot_general(a, b, (((1,), (1,)), ((), ())), preferred_element_type=F32)


def norm(xv):
    mean = jnp.mean(xv, axis=-1, keepdims=True)
    cen = xv - mean
    var = jnp.mean(cen * cen, axis=-1, keepdims=True)
    return cen * lax.rsqrt(var + 1e-6)


def gelu(hv):
    inner = 0.7978845608028654 * (hv + 0.044715 * (hv * hv * hv))
    return 0.5 * hv * (1.0 + jnp.tanh(inner))


def roles(mesh_tokens, mesh_frames):
    tok, frm = lax.axis_index("tokens"), lax.axis_index("frames")
    chip, core = frm // 2, frm % 2
    odd = (tok // 2 + chip) % 2
    half = ((tok + 1) // 2) % 2
    return tok, frm, chip, core, odd, half


def kernel(cfg, z_in, mod, noise, bias, w_in, w_out, sqkv_h, so_h, tqkv_h, to_h, up_h, down_h, z, emit,
           x, ust, us, kvs, qs, obuf, osnd, ut, utr, qt, kt, vt, sc, pb, bm, ob, uu, hb,
           sqkv, so, tqkv, to, up, down,
           us_s, us_r, o_s, o_r, ut_s, ut_r, w_sem, credit):
    L, S, NC, CH, TK, D, FF, HD, MT, MF, WIN = cfg
    R, HS, RH, G = CH * TK, CH // 2, CH * TK // 2, TK // SUB
    CR = CH * SUB
    SR = NC * CH * SUB
    NT = L * S
    HP = D // LANES
    W = min(256, D)
    DT = D // W
    FT = min(256, FF)
    qscale = HD ** -0.5

    vid = lax.axis_index("videos")
    tok, frm, chip, core, odd, _ = roles(MT, MF)
    sib_f = frm + 1 - 2 * core
    par_t = tok + 1 - 2 * (tok % 2)
    block = chip * 2 + odd
    first = block == 0
    sib = (vid, tok, sib_f)
    par_a = (vid, par_t, frm)
    par_b = (vid, par_t, sib_f)
    nxt = (vid, jnp.where(odd == 0, MT - 1 - tok, tok), jnp.where(odd == 0, frm, (frm + 2) % MF))
    prv = (vid, jnp.where(odd == 1, MT - 1 - tok, tok), jnp.where(odd == 1, frm, (frm + MF - 2) % MF))

    def w_copy(k, layer):
        src, dst = ((sqkv_h, sqkv), (so_h, so), (to_h, to), (up_h, up), (down_h, down))[k]
        return pltpu.make_async_copy(src.at[layer], dst, w_sem.at[k])

    def t_copy(layer):
        return pltpu.make_async_copy(tqkv_h.at[layer], tqkv.at[layer], w_sem.at[5 + layer])

    w_copy(0, 0).start()
    w_copy(1, 0).start()
    for layer in range(L):
        t_copy(layer).start()

    barrier = pltpu.get_barrier_semaphore()
    for dev in (sib, par_a, par_b, nxt, prv):
        pl.semaphore_signal(barrier, inc=1, device_id=dev, device_id_type=MESH)
    pl.semaphore_wait(barrier, 5)

    def remote(src, dst, ss, rs, dev):
        return pltpu.make_async_remote_copy(src_ref=src, dst_ref=dst, send_sem=ss, recv_sem=rs, device_id=dev, device_id_type=MESH)

    def us_copies(par, i):
        return (
            remote(ust.at[i, 1 - core], us.at[par, i, 0], us_s.at[i, 0], us_r.at[par, i, 0], sib),
            remote(ust.at[i, core], us.at[par, i, 1], us_s.at[i, 1], us_r.at[par, i, 1], par_a),
            remote(ust.at[i, 1 - core], us.at[par, i, 2], us_s.at[i, 2], us_r.at[par, i, 2], par_b),
        )

    def o_copy(i):
        return remote(osnd.at[i], obuf.at[i, core], o_s.at[i], o_r.at[i], sib)

    def ut_copy(par, i):
        return remote(ut.at[i], utr.at[par, i], ut_s.at[i], ut_r.at[par, i], nxt)

    z[...] = z_in[...]
    emit[...] = jnp.zeros_like(emit)
    for g in range(G):
        for ref in (kt, vt):
            ref[g] = jnp.zeros(ref.shape[1:], BF)

    lane = lax.broadcasted_iota(jnp.int32, (1, LANES), 1)
    low = lane < HD

    def stack_heads(q):
        zero = jnp.zeros_like(q)
        return jnp.concatenate([jnp.where(low, q, zero), jnp.where(low, zero, q)], axis=0)

    def softmax_rows(sv):
        top = jnp.max(sv, axis=-1, keepdims=True)
        e = jnp.exp(sv - top)
        return (e * (1.0 / jnp.sum(e, axis=-1, keepdims=True))).astype(BF)

    def modulated(i, a, layer, step, which):
        row = i * CH + a + (S - 1) - step
        shift = mod[row, pl.ds(layer * 6 + 2 * which, 1), :]
        scale = mod[row, pl.ds(layer * 6 + 2 * which + 1, 1), :]
        xv = x[i, pl.ds(a * TK, TK), :]
        return (norm(xv) * (1.0 + scale) + shift).astype(BF)

    def spatial(i, par):
        for c in us_copies(par, i):
            c.wait()
        own = ust[i, core]
        u_all = jnp.concatenate([own, us[par, i, 0], us[par, i, 1], us[par, i, 2]], axis=0)
        u_q = jnp.concatenate([own, us[par, i, 0]], axis=0)
        for t in range(DT):
            y = (mm(u_q, sqkv[:, t * W:(t + 1) * W]) * qscale).astype(BF)
            for p in range(2):
                for s in range(HS):
                    qs[s, p * TK:(p + 1) * TK, t * W:(t + 1) * W] = y[p * RH + s * TK:p * RH + (s + 1) * TK]
        for t in range(2 * DT):
            y = mm(u_all, sqkv[:, D + t * W:D + (t + 1) * W]).astype(BF)
            for p in range(4):
                for s in range(HS):
                    kvs[s, p * TK:(p + 1) * TK, t * W:(t + 1) * W] = y[p * RH + s * TK:p * RH + (s + 1) * TK]

        @pl.loop(0, HS)
        def _(s):
            for h in range(HP):
                cols = slice(h * LANES, (h + 1) * LANES)
                sc[h, 0:4 * TK, 0:4 * TK] = mm_t(stack_heads(qs[s, :, cols]), kvs[s, :, cols])
            for h in range(HP):
                pb[h, 0:4 * TK, 0:4 * TK] = softmax_rows(sc[h, 0:4 * TK, 0:4 * TK])
            for h in range(HP):
                cols = slice(h * LANES, (h + 1) * LANES)
                o2 = mm(pb[h, 0:4 * TK, 0:4 * TK], kvs[s, :, D + h * LANES:D + (h + 1) * LANES])
                o = jnp.where(low, o2[:2 * TK], o2[2 * TK:]).astype(BF)
                rows = pl.ds(pl.multiple_of(s * TK, TK), TK)
                obuf[i, core, rows, cols] = o[:TK]
                osnd[i, rows, cols] = o[TK:]

        o_copy(i).start()

    def project(i, par, layer, step, n):
        o_copy(i).wait()
        ov = obuf[i].reshape(R, D)
        for t in range(DT):
            cols = slice(t * W, (t + 1) * W)
            x[i, :, cols] = x[i, :, cols] + mm(ov, so[:, cols])
        for a in range(CH):
            ut[i, a * TK:(a + 1) * TK, :] = modulated(i, a, layer, step, 1)

        @pl.when((i == NC - 1) & (n >= 2))
        def _():
            pl.semaphore_wait(credit, 1)

        ut_copy(par, i).start()
        uv = ut[i]
        for t in range(3 * DT):
            y = mm(uv, tqkv[layer, :, t * W:(t + 1) * W])
            kind, tt = t // DT, t % DT
            if kind == 0:
                y = y * qscale
            y4 = y.reshape(CH, G, SUB, W)
            for g in range(G):
                yg = y4[:, g].reshape(CR, W).astype(BF)
                if kind == 0:
                    qt[g, pl.ds(pl.multiple_of(i * CR, CR), CR), tt * W:(tt + 1) * W] = yg
                else:
                    ref = kt if kind == 1 else vt
                    ref[g, pl.ds(pl.multiple_of(SR + i * CR, CR), CR), tt * W:(tt + 1) * W] = yg

    def temporal(i, par, layer, step):
        ut_copy(par, i).wait()
        uv = utr[par, i]
        for t in range(2 * DT):
            y = mm(uv, tqkv[layer, :, D + t * W:D + (t + 1) * W])
            kind, tt = t // DT, t % DT
            ref = vt if kind else kt
            y4 = y.reshape(CH, G, SUB, W)
            for g in range(G):
                ref[g, pl.ds(pl.multiple_of(i * CR, CR), CR), tt * W:(tt + 1) * W] = y4[:, g].reshape(CR, W).astype(BF)
        rows = lax.broadcasted_iota(jnp.int32, (2 * CR, WIN), 0)
        keys = lax.broadcasted_iota(jnp.int32, (2 * CR, WIN), 1)
        pos_q = i * CH + (rows & (CR - 1)) // SUB
        pos_k = (i - NC) * CH + keys // SUB
        pos = block * NC * CH + pos_q - step
        slot = jnp.where(pos < 0, pos + MF * NC * CH, pos)
        valid = pos_q - pos_k <= slot
        for h in range(HP):
            bm[h] = jnp.where(valid, bias[layer, h], -jnp.inf)

        @pl.loop(0, G // 2)
        def _(gg):
            qrows = pl.ds(pl.multiple_of(i * CR, CR), CR)
            krows = pl.ds(pl.multiple_of(i * CR, CR), WIN)
            units = [(gg * 2 + d, d * 2 * CR, h) for d in range(2) for h in range(HP)]
            for g, r, h in units:
                cols = slice(h * LANES, (h + 1) * LANES)
                sc[h, r:r + 2 * CR, 0:WIN] = mm_t(stack_heads(qt[g, qrows, cols]), kt[g, krows, cols]) + bm[h]
            for g, r, h in units:
                pb[h, r:r + 2 * CR, 0:WIN] = softmax_rows(sc[h, r:r + 2 * CR, 0:WIN])
            for g, r, h in units:
                cols = slice(h * LANES, (h + 1) * LANES)
                o2 = mm(pb[h, r:r + 2 * CR, 0:WIN], vt[g, krows, cols])
                ob[pl.ds(pl.multiple_of(g * CR, CR), CR), cols] = jnp.where(low, o2[:CR], o2[CR:]).astype(BF)

        ov = ob[...]
        for t in range(DT):
            cols = slice(t * W, (t + 1) * W)
            y4 = mm(ov, to[:, cols]).reshape(G, CH, SUB, W)
            for a in range(CH):
                x[i, a * TK:(a + 1) * TK, cols] = x[i, a * TK:(a + 1) * TK, cols] + y4[:, a].reshape(TK, W)

    def mlp(i, layer, step):
        for a in range(CH):
            uu[a * TK:(a + 1) * TK, :] = modulated(i, a, layer, step, 2)
        uv = uu[...]
        for t in range(FF // FT):
            hp = mm(uv, up[:, t * FT:(t + 1) * FT])
            for r in range(0, R, 128):
                hb[r:r + 128, t * FT:(t + 1) * FT] = gelu(hp[r:r + 128]).astype(BF)
        for t in range(DT):
            cols = slice(t * W, (t + 1) * W)
            for r in range(0, R, 256):
                x[i, r:r + 256, cols] = x[i, r:r + 256, cols] + mm(hb[r:r + 256], down[:, cols])

    def finish(i, step):
        for a in range(CH):
            uu[a * TK:(a + 1) * TK, :] = norm(x[i, a * TK:(a + 1) * TK, :]).astype(BF)
        v = mm(uu[...], w_out[...])
        for a in range(CH):
            row = i * CH + a + (S - 1) - step
            dt = mod[row, pl.ds(6 * L, 1), 0:LANES]
            z[i, a * TK:(a + 1) * TK, :] = z[i, a * TK:(a + 1) * TK, :] + dt * v[a * TK:(a + 1) * TK]

        @pl.when(i == step // CH)
        def _():
            rows = pl.ds(pl.multiple_of((step % CH) * TK, TK), TK)
            zv = z[i, rows, :]
            emit[step] = zv
            z[i, rows, :] = jnp.where(first, noise[step], zv)

    def enter(i):
        x[i] = mm(z[i].astype(BF), w_in[...]).astype(BF).astype(F32)

    def launch(i, par, layer, step):
        for a in range(CH):
            ust[i, a // HS, (a % HS) * TK:(a % HS + 1) * TK, :] = modulated(i, a, layer, step, 0)
        for c in us_copies(par, i):
            c.start()

    @pl.loop(0, NT + 1)
    def _(m):
        n = m - 1
        layer, step, par = lax.rem(n + L, L), (n + L) // L - 1, lax.rem(n + 2, 2)
        nlayer, nstep, npar = lax.rem(m, L), m // L, lax.rem(m, 2)

        @pl.when(m > 0)
        def _():
            w_copy(0, layer).wait()
            w_copy(1, layer).wait()

            @pl.when(m == 1)
            def _():
                for q in range(L):
                    t_copy(q).wait()

            for k in (2, 3, 4):
                w_copy(k, layer).start()

            @pl.loop(0, NC)
            def _(c):
                spatial(NC - 1 - c, par)
                project(NC - 1 - c, par, layer, step, n)

            for k in (2, 3, 4):
                w_copy(k, layer).wait()

            @pl.when(m < NT)
            def _():
                w_copy(0, nlayer).start()
                w_copy(1, nlayer).start()

        @pl.loop(0, NC)
        def _(c):
            i = NC - 1 - c

            @pl.when(m > 0)
            def _():
                temporal(i, par, layer, step)
                mlp(i, layer, step)

                @pl.when(layer == L - 1)
                def _():
                    finish(i, step)

            @pl.when(m < NT)
            def _():
                @pl.when(nlayer == 0)
                def _():
                    enter(i)

                launch(i, npar, nlayer, nstep)

        @pl.when(m > 0)
        def _():
            pl.semaphore_signal(credit, inc=1, device_id=prv, device_id_type=MESH)

    pl.semaphore_wait(credit, min(2, NT))


def denoise_call(cfg, vmem, *args):
    L, S, NC, CH, TK, D, FF, HD, MT, MF, WIN = cfg
    R, HS, RH, G = CH * TK, CH // 2, CH * TK // 2, TK // SUB
    CR, SR = CH * SUB, NC * CH * SUB
    HP = D // LANES
    KR = (NC - 1) * CR + WIN
    scr = [
        pltpu.VMEM((NC, R, D), F32),
        pltpu.VMEM((NC, 2, RH, D), BF),
        pltpu.VMEM((2, NC, 3, RH, D), BF),
        pltpu.VMEM((HS, 4 * TK, 2 * D), BF),
        pltpu.VMEM((HS, 2 * TK, D), BF),
        pltpu.VMEM((NC, 2, RH, D), BF),
        pltpu.VMEM((NC, RH, D), BF),
        pltpu.VMEM((NC, R, D), BF),
        pltpu.VMEM((2, NC, R, D), BF),
        pltpu.VMEM((G, SR, D), BF),
        pltpu.VMEM((G, KR, D), BF),
        pltpu.VMEM((G, KR, D), BF),
        pltpu.VMEM((HP, max(4 * TK, 4 * CR), max(4 * TK, WIN)), F32),
        pltpu.VMEM((HP, max(4 * TK, 4 * CR), max(4 * TK, WIN)), BF),
        pltpu.VMEM((HP, 2 * CR, WIN), F32),
        pltpu.VMEM((R, D), BF),
        pltpu.VMEM((R, D), BF),
        pltpu.VMEM((R, FF), BF),
        pltpu.VMEM((D, 3 * D), BF),
        pltpu.VMEM((D, D), BF),
        pltpu.VMEM((L, D, 3 * D), BF),
        pltpu.VMEM((D, D), BF),
        pltpu.VMEM((D, FF), BF),
        pltpu.VMEM((FF, D), BF),
        pltpu.SemaphoreType.DMA((NC, 3)),
        pltpu.SemaphoreType.DMA((2, NC, 3)),
        pltpu.SemaphoreType.DMA((NC,)),
        pltpu.SemaphoreType.DMA((NC,)),
        pltpu.SemaphoreType.DMA((NC,)),
        pltpu.SemaphoreType.DMA((2, NC)),
        pltpu.SemaphoreType.DMA((5 + L,)),
        pltpu.SemaphoreType.REGULAR,
    ]
    inner = pl.BlockSpec(memory_space=pltpu.VMEM)
    outer = pl.BlockSpec(memory_space=pl.ANY)
    return pl.pallas_call(
        functools.partial(kernel, cfg),
        out_shape=(jax.ShapeDtypeStruct((NC, R, LANES), F32), jax.ShapeDtypeStruct((S, TK, LANES), F32)),
        in_specs=[inner] * 6 + [outer] * 6,
        out_specs=(inner, inner),
        scratch_shapes=scr,
        compiler_params=pltpu.CompilerParams(collective_id=0, has_side_effects=True, vmem_limit_bytes=vmem),
        name="fifo_denoise",
    )(*args)


def lag_bias_tiles(lag_bias, CH, SLOTS, WIN):
    L, H, window = lag_bias.shape
    a = jnp.arange(CH)[:, None, None, None]
    tq = jnp.arange(SUB)[None, :, None, None]
    k = jnp.arange(WIN // SUB)[None, None, :, None]
    tk = jnp.arange(SUB)[None, None, None, :]
    lag = SLOTS + a - k
    ok = (lag >= 0) & (lag < window) & (tq == tk)
    tiles = jnp.where(ok, jnp.take(lag_bias, jnp.clip(lag, 0, window - 1), axis=2), -jnp.inf)
    return tiles.reshape(L, H // 2, 2 * CH * SUB, WIN)


def solution(mesh):
    MT, MF = mesh.shape["tokens"], mesh.shape["frames"]
    slot_spec = P(("videos", "frames"), "tokens", None)
    mod_spec = P(("videos", "frames"), None, None, None)
    step_spec = P(("videos", "frames"))
    noise_spec = P("videos", "tokens", None)
    emit_spec = P("videos", ("tokens", "frames"), None)
    to_sib = [(f, f ^ 1) for f in range(MF)]
    to_next_chip = [(f, (f + 2) % MF) for f in range(MF)]

    def body(z_loc, mod_loc, step_loc, noise_loc, lag_bias, w_in, w_out, w_sqkv, w_so, w_tqkv, w_to, w_up, w_down):
        SL, TK, C = z_loc.shape
        S = noise_loc.shape[0]
        L, D, FF = w_up.shape
        HD = w_so.shape[2]
        NC = CHUNKS
        CH = SL // NC
        WIN = 2 * SL * SUB
        tok, frm, chip, core, odd, half = roles(MT, MF)
        quarter = 2 * half + core

        zn = jnp.concatenate([z_loc.reshape(SL, TK * C), noise_loc.reshape(S, TK * C)], axis=0)
        zn = lax.all_gather(zn, "tokens", axis=0)
        zq = lax.dynamic_index_in_dim(zn, quarter, axis=0, keepdims=False)
        sent = lax.dynamic_index_in_dim(zn, 2 * half + (1 - core), axis=0, keepdims=False)[:SL]
        z_sib = lax.ppermute(sent, "frames", to_sib)
        z_own = jnp.where(odd == core, zq[:SL], z_sib).reshape(SL, TK, C)
        noise = zq[SL:].reshape(S, TK, C)
        pad = lambda v: jnp.pad(v, ((0, 0),) * (v.ndim - 1) + ((0, LANES - C),))

        table = jnp.concatenate([mod_loc.reshape(SL, L * 6, D), jnp.broadcast_to(step_loc[:, None, None], (SL, 1, D))], axis=1)
        table_sib = lax.ppermute(table, "frames", to_sib)
        even_blk = jnp.where(core == 0, table, table_sib)
        odd_blk = jnp.where(core == 1, table, table_sib)
        tail = lax.ppermute(odd_blk[SL - (S - 1):], "frames", to_next_chip)
        own_tab = jnp.where(odd == 0, even_blk, odd_blk)
        prev_tab = jnp.where(odd == 0, tail, even_blk[SL - (S - 1):])
        mod = jnp.concatenate([prev_tab, own_tab], axis=0)

        cfg = (L, S, NC, CH, TK, D, FF, HD, MT, MF, WIN)
        z_new, emit = denoise_call(
            cfg, 67043328,
            pad(z_own).reshape(NC, CH * TK, LANES), mod, pad(noise), lag_bias_tiles(lag_bias, CH, SL, WIN),
            jnp.pad(w_in, ((0, LANES - C), (0, 0))), jnp.pad(w_out, ((0, 0), (0, LANES - C))),
            w_sqkv.reshape(L, D, 3 * D), w_so.reshape(L, D, D), w_tqkv.reshape(L, D, 3 * D), w_to.reshape(L, D, D), w_up, w_down,
        )

        mine = jnp.concatenate([z_new.reshape(SL, TK, LANES)[:, :, :C].reshape(SL, TK * C), emit[:, :, :C].reshape(S, TK * C)], axis=0)
        every = lax.all_gather(mine, ("tokens", "frames"), axis=0)
        where_is = []
        for blk in range(MF):
            for q in range(MT):
                xx, o, hf, cc = blk // 2, blk % 2, q // 2, q % 2
                ty = [t for t in range(MT) if (t // 2 + xx) % 2 == o and ((t + 1) // 2) % 2 == hf]
                where_is.append(ty[0] * MF + 2 * xx + cc)
        queue = jnp.stack([every[d, :SL] for d in where_is]).reshape(MF, MT, SL, TK * C)
        queue = jnp.roll(jnp.swapaxes(queue, 1, 2).reshape(MF * SL, MT, TK * C), -S, axis=0)
        z_fin = lax.dynamic_slice(queue, (frm * SL, tok, 0), (SL, 1, TK * C)).reshape(SL, TK, C)
        em = jnp.stack([every[where_is[q], SL:] for q in range(MT)])
        per = TK // MF
        em = lax.dynamic_slice(em, (tok, 0, frm * per * C), (1, S, per * C)).reshape(S, per, C)
        return em, z_fin

    return jax.shard_map(body, mesh=mesh, in_specs=(slot_spec, mod_spec, step_spec, noise_spec) + (P(),) * 9, out_specs=(emit_spec, slot_spec), check_vma=False)
```

```python
import functools

import jax
import jax.numpy as jnp
from jax import lax
from jax.experimental import pallas as pl
from jax.experimental.pallas import tpu as pltpu
from jax.sharding import PartitionSpec as P

MESH = pl.DeviceIdType.MESH
BF = jnp.bfloat16
F32 = jnp.float32
LANES = 128
SUB = 8
CHUNKS = 4


def mm(a, b):
    return jnp.dot(a, b, preferred_element_type=F32)


def mm_t(a, b):
    return lax.dot_general(a, b, (((1,), (1,)), ((), ())), preferred_element_type=F32)


def norm(xv):
    mean = jnp.mean(xv, axis=-1, keepdims=True)
    cen = xv - mean
    var = jnp.mean(cen * cen, axis=-1, keepdims=True)
    return cen * lax.rsqrt(var + 1e-6)


def gelu(hv):
    inner = 0.7978845608028654 * (hv + 0.044715 * (hv * hv * hv))
    return 0.5 * hv * (1.0 + jnp.tanh(inner))


def roles(mesh_tokens, mesh_frames):
    tok, frm = lax.axis_index("tokens"), lax.axis_index("frames")
    chip, core = frm // 2, frm % 2
    odd = (tok // 2 + chip) % 2
    half = ((tok + 1) // 2) % 2
    return tok, frm, chip, core, odd, half


def kernel(cfg, lag_bias, z_in, noise, w_in, w_out, own_tab, prev_tab, sqkv_h, so_h, tqkv_h, to_h, up_h, down_h, z, emit,
           mod, bias, x, ust, us, kvs, qs, obuf, osnd, ut, utr, qt, kt, vt, pb, bm, ob, uu, hb,
           sqkv, so, tqkv, to, up, down,
           us_s, us_r, o_s, o_r, ut_s, ut_r, w_sem, t_sem, credit):
    L, S, NC, CH, TK, D, FF, HD, MT, MF, WIN = cfg
    R, HS, RH, G = CH * TK, CH // 2, CH * TK // 2, TK // SUB
    CR = CH * SUB
    SR = NC * CH * SUB
    NT = L * S
    HP = D // LANES
    W = min(256, D)
    DT = D // W
    FT = min(256, FF)
    qscale = HD ** -0.5
    SU, TU, RS = min(2, HS), min(4, G), min(64, 4 * TK)

    vid = lax.axis_index("videos")
    tok, frm, chip, core, odd, _ = roles(MT, MF)
    sib_f = frm + 1 - 2 * core
    par_t = tok + 1 - 2 * (tok % 2)
    block = chip * 2 + odd
    first = block == 0
    sib = (vid, tok, sib_f)
    par_a = (vid, par_t, frm)
    par_b = (vid, par_t, sib_f)
    nxt = (vid, jnp.where(odd == 0, MT - 1 - tok, tok), jnp.where(odd == 0, frm, (frm + 2) % MF))
    prv = (vid, jnp.where(odd == 1, MT - 1 - tok, tok), jnp.where(odd == 1, frm, (frm + MF - 2) % MF))

    def w_copy(k, layer):
        src, dst = ((sqkv_h, sqkv), (so_h, so), (to_h, to), (up_h, up), (down_h, down))[k]
        return pltpu.make_async_copy(src.at[layer], dst, w_sem.at[k])

    def t_copy(layer):
        return pltpu.make_async_copy(tqkv_h.at[layer], tqkv.at[layer], w_sem.at[5 + layer])

    tables = (
        pltpu.make_async_copy(prev_tab, mod.at[0:S - 1], t_sem.at[0]),
        pltpu.make_async_copy(own_tab, mod.at[S - 1:S - 1 + NC * CH], t_sem.at[1]),
    )
    for c in tables:
        c.start()
    w_copy(0, 0).start()
    w_copy(1, 0).start()
    for layer in range(L):
        t_copy(layer).start()

    barrier = pltpu.get_barrier_semaphore()
    for dev in (sib, par_a, par_b, nxt, prv):
        pl.semaphore_signal(barrier, inc=1, device_id=dev, device_id_type=MESH)
    pl.semaphore_wait(barrier, 5)

    def remote(src, dst, ss, rs, dev):
        return pltpu.make_async_remote_copy(src_ref=src, dst_ref=dst, send_sem=ss, recv_sem=rs, device_id=dev, device_id_type=MESH)

    def us_copies(par, i):
        return (
            remote(ust.at[i, 1 - core], us.at[par, i, 0], us_s.at[i, 0], us_r.at[par, i, 0], sib),
            remote(ust.at[i, core], us.at[par, i, 1], us_s.at[i, 1], us_r.at[par, i, 1], par_a),
            remote(ust.at[i, 1 - core], us.at[par, i, 2], us_s.at[i, 2], us_r.at[par, i, 2], par_b),
        )

    def o_copy(i):
        return remote(osnd.at[i], obuf.at[i, core], o_s.at[i], o_r.at[i], sib)

    def ut_copy(par, i):
        return remote(ut.at[i], utr.at[par, i], ut_s.at[i], ut_r.at[par, i], nxt)

    z[...] = z_in[...]
    emit[...] = jnp.zeros_like(emit)
    for g in range(G):
        for ref in (kt, vt):
            ref[g] = jnp.zeros(ref.shape[1:], BF)

    q_row = lax.broadcasted_iota(jnp.int32, (CR, WIN), 0)
    k_col = lax.broadcasted_iota(jnp.int32, (CR, WIN), 1)
    lag = NC * CH + q_row // SUB - k_col // SUB
    lag = jnp.where((q_row & (SUB - 1)) == (k_col & (SUB - 1)), lag, -1)

    @pl.loop(0, L * HP)
    def _(lh):
        for hd in range(2):
            tile = jnp.full((CR, WIN), -jnp.inf, F32)
            for r in range(lag_bias.shape[1]):
                tile = jnp.where(lag == r, lag_bias[2 * lh + hd, r], tile)
            bias[lh // HP, lh % HP, hd * CR:(hd + 1) * CR, :] = tile

    for c in tables:
        c.wait()

    lane = lax.broadcasted_iota(jnp.int32, (1, LANES), 1)
    low = lane < HD

    def stack_heads(q):
        zero = jnp.zeros_like(q)
        return jnp.concatenate([jnp.where(low, q, zero), jnp.where(low, zero, q)], axis=0)

    def softmax_rows(sv):
        top = jnp.max(sv, axis=-1, keepdims=True)
        e = jnp.exp(sv - top)
        return (e * (1.0 / jnp.sum(e, axis=-1, keepdims=True))).astype(BF)

    NR = min(32, TK)

    def modulated(i, a, layer, step, which, put):
        row = i * CH + a + (S - 1) - step
        shift = mod[row, pl.ds(2 * which * L + layer, 1), :]
        gain = 1.0 + mod[row, pl.ds((2 * which + 1) * L + layer, 1), :]
        for r in range(0, TK, NR):
            xv = x[i, a * TK + r:a * TK + r + NR, :]
            put(r, (norm(xv) * gain + shift).astype(BF))

    def spatial(i, par):
        for c in us_copies(par, i):
            c.wait()
        own = ust[i, core]
        u_all = jnp.concatenate([own, us[par, i, 0], us[par, i, 1], us[par, i, 2]], axis=0)
        u_q = jnp.concatenate([own, us[par, i, 0]], axis=0)
        for t in range(DT):
            y = (mm_t(u_q, sqkv[t * W:(t + 1) * W, :]) * qscale).astype(BF)
            for p in range(2):
                for s in range(HS):
                    qs[s, p * TK:(p + 1) * TK, t * W:(t + 1) * W] = y[p * RH + s * TK:p * RH + (s + 1) * TK]
        for t in range(2 * DT):
            y = mm_t(u_all, sqkv[D + t * W:D + (t + 1) * W, :]).astype(BF)
            for p in range(4):
                for s in range(HS):
                    kvs[s, p * TK:(p + 1) * TK, t * W:(t + 1) * W] = y[p * RH + s * TK:p * RH + (s + 1) * TK]

        @pl.loop(0, HS // SU)
        def _(ss):
            units = [(ss * SU + d, d * HP + h, h) for d in range(SU) for h in range(HP)]
            for s, p, h in units:
                cols = slice(h * LANES, (h + 1) * LANES)
                sv = mm_t(stack_heads(qs[s, :, cols]), kvs[s, :, cols])
                for r in range(0, 4 * TK, RS):
                    pb[p, r:r + RS, 0:4 * TK] = softmax_rows(sv[r:r + RS])
            for s, p, h in units:
                cols = slice(h * LANES, (h + 1) * LANES)
                o2 = mm(pb[p, 0:4 * TK, 0:4 * TK], kvs[s, :, D + h * LANES:D + (h + 1) * LANES])
                o = jnp.where(low, o2[:2 * TK], o2[2 * TK:]).astype(BF)
                rows = pl.ds(pl.multiple_of(s * TK, TK), TK)
                obuf[i, core, rows, cols] = o[:TK]
                osnd[i, rows, cols] = o[TK:]

        o_copy(i).start()

    def project(i, par, layer, step, n):
        o_copy(i).wait()
        ov = obuf[i].reshape(R, D)
        for r in range(0, R, R // 2):
            for t in range(DT):
                cols = slice(t * W, (t + 1) * W)
                x[i, r:r + R // 2, cols] = x[i, r:r + R // 2, cols] + mm(ov[r:r + R // 2], so[:, cols])
        for a in range(CH):
            def put(r, v, a=a):
                ut[i, a * TK + r:a * TK + r + NR, :] = v

            modulated(i, a, layer, step, 1, put)

        @pl.when((i == NC - 1) & (n >= 2))
        def _():
            pl.semaphore_wait(credit, 1)

        ut_copy(par, i).start()

    def own_qkv(i, layer):
        uv = ut[i]
        for t in range(3 * DT):
            y = mm_t(uv, tqkv[layer, t * W:(t + 1) * W, :])
            kind, tt = t // DT, t % DT
            if kind == 0:
                y = y * qscale
            y4 = y.reshape(CH, G, SUB, W)
            for g in range(G):
                yg = y4[:, g].reshape(CR, W).astype(BF)
                if kind == 0:
                    qt[g, pl.ds(pl.multiple_of(i * CR, CR), CR), tt * W:(tt + 1) * W] = yg
                else:
                    ref = kt if kind == 1 else vt
                    ref[g, pl.ds(pl.multiple_of(SR + i * CR, CR), CR), tt * W:(tt + 1) * W] = yg

    def temporal(i, par, layer, step):
        ut_copy(par, i).wait()
        uv = utr[par, i]
        for t in range(2 * DT):
            y = mm_t(uv, tqkv[layer, D + t * W:D + (t + 1) * W, :])
            kind, tt = t // DT, t % DT
            ref = vt if kind else kt
            y4 = y.reshape(CH, G, SUB, W)
            for g in range(G):
                ref[g, pl.ds(pl.multiple_of(i * CR, CR), CR), tt * W:(tt + 1) * W] = y4[:, g].reshape(CR, W).astype(BF)
        rows = lax.broadcasted_iota(jnp.int32, (2 * CR, WIN), 0)
        keys = lax.broadcasted_iota(jnp.int32, (2 * CR, WIN), 1)
        pos_q = i * CH + (rows & (CR - 1)) // SUB
        pos_k = (i - NC) * CH + keys // SUB
        pos = block * NC * CH + pos_q - step
        slot = jnp.where(pos < 0, pos + MF * NC * CH, pos)
        valid = pos_q - pos_k <= slot
        for h in range(HP):
            bm[h] = jnp.where(valid, bias[layer, h], -jnp.inf)

        @pl.loop(0, G // TU)
        def _(gg):
            qrows = pl.ds(pl.multiple_of(i * CR, CR), CR)
            krows = pl.ds(pl.multiple_of(i * CR, CR), WIN)
            units = [(gg * TU + d, d * 2 * CR, h) for d in range(TU) for h in range(HP)]
            for g, r, h in units:
                cols = slice(h * LANES, (h + 1) * LANES)
                sv = mm_t(stack_heads(qt[g, qrows, cols]), kt[g, krows, cols]) + bm[h]
                pb[h, r:r + 2 * CR, 0:WIN] = softmax_rows(sv)
            for g, r, h in units:
                cols = slice(h * LANES, (h + 1) * LANES)
                o2 = mm(pb[h, r:r + 2 * CR, 0:WIN], vt[g, krows, cols])
                ob[pl.ds(pl.multiple_of(g * CR, CR), CR), cols] = jnp.where(low, o2[:CR], o2[CR:]).astype(BF)

        ov = ob[...]
        for r in range(0, R, R // 2):
            for t in range(DT):
                cols = slice(t * W, (t + 1) * W)
                r0, r1 = r, r + R // 2
                g0, gn = r0 // CR, (r1 - r0) // CR
                y4 = mm(ov[r0:r1], to[:, cols]).reshape(gn, CH, SUB, W)
                for a in range(CH):
                    rows = slice(a * TK + g0 * SUB, a * TK + (g0 + gn) * SUB)
                    x[i, rows, cols] = x[i, rows, cols] + y4[:, a].reshape(gn * SUB, W)

    def mlp(i, layer, step):
        for a in range(CH):
            def put(r, v, a=a):
                uu[a * TK + r:a * TK + r + NR, :] = v

            modulated(i, a, layer, step, 2, put)
        uv = uu[...]
        for t in range(FF // FT):
            hp = mm(uv, up[:, t * FT:(t + 1) * FT])
            for r in range(0, R, min(R, 128)):
                hb[r:r + 128, t * FT:(t + 1) * FT] = gelu(hp[r:r + 128]).astype(BF)
        for r in range(0, R, R // 2):
            for t in range(DT):
                cols = slice(t * W, (t + 1) * W)
                x[i, r:r + R // 2, cols] = x[i, r:r + R // 2, cols] + mm(hb[r:r + R // 2], down[:, cols])

    def finish(i, step):
        for r in range(0, R, NR):
            uu[r:r + NR, :] = norm(x[i, r:r + NR, :]).astype(BF)
        v = mm(uu[...], w_out[...])
        for a in range(CH):
            row = i * CH + a + (S - 1) - step
            dt = mod[row, pl.ds(6 * L, 1), 0:LANES]
            z[i, a * TK:(a + 1) * TK, :] = z[i, a * TK:(a + 1) * TK, :] + dt * v[a * TK:(a + 1) * TK]

        @pl.when(i == step // CH)
        def _():
            rows = pl.ds(pl.multiple_of((step % CH) * TK, TK), TK)
            zv = z[i, rows, :]
            emit[step] = zv
            z[i, rows, :] = jnp.where(first, noise[step], zv)

    def enter(i):
        x[i] = mm(z[i].astype(BF), w_in[...]).astype(BF).astype(F32)

    def launch(i, par, layer, step):
        for a in range(CH):
            def put(r, v, a=a):
                ust[i, a // HS, (a % HS) * TK + r:(a % HS) * TK + r + NR, :] = v

            modulated(i, a, layer, step, 0, put)
        for c in us_copies(par, i):
            c.start()

    @pl.loop(0, NT + 1)
    def _(m):
        n = m - 1
        layer, step, par = lax.rem(n + L, L), (n + L) // L - 1, lax.rem(n + 2, 2)
        nlayer, nstep, npar = lax.rem(m, L), m // L, lax.rem(m, 2)

        @pl.when(m > 0)
        def _():
            w_copy(0, layer).wait()
            w_copy(1, layer).wait()

            @pl.when(m == 1)
            def _():
                for q in range(L):
                    t_copy(q).wait()

            for k in (2, 3, 4):
                w_copy(k, layer).start()

            @pl.loop(0, NC + 1)
            def _(c):
                @pl.when(c < NC)
                def _():
                    spatial(NC - 1 - c, par)

                @pl.when(c > 0)
                def _():
                    own_qkv(NC - c, layer)

                @pl.when(c < NC)
                def _():
                    project(NC - 1 - c, par, layer, step, n)

            for k in (2, 3, 4):
                w_copy(k, layer).wait()

            @pl.when(m < NT)
            def _():
                w_copy(0, nlayer).start()
                w_copy(1, nlayer).start()

        @pl.loop(0, NC)
        def _(c):
            i = NC - 1 - c

            @pl.when(m > 0)
            def _():
                temporal(i, par, layer, step)
                mlp(i, layer, step)

                @pl.when(layer == L - 1)
                def _():
                    finish(i, step)

            @pl.when(m < NT)
            def _():
                @pl.when(nlayer == 0)
                def _():
                    enter(i)

                launch(i, npar, nlayer, nstep)

        @pl.when(m > 0)
        def _():
            pl.semaphore_signal(credit, inc=1, device_id=prv, device_id_type=MESH)

    pl.semaphore_wait(credit, min(2, NT))


def denoise_call(cfg, vmem, *args):
    L, S, NC, CH, TK, D, FF, HD, MT, MF, WIN = cfg
    R, HS, RH, G = CH * TK, CH // 2, CH * TK // 2, TK // SUB
    CR, SR = CH * SUB, NC * CH * SUB
    HP = D // LANES
    KR = (NC - 1) * CR + WIN
    scr = [
        pltpu.VMEM((S - 1 + NC * CH, 6 * L + 1, D), F32),
        pltpu.VMEM((L, HP, 2 * CR, WIN), F32),
        pltpu.VMEM((NC, R, D), F32),
        pltpu.VMEM((NC, 2, RH, D), BF),
        pltpu.VMEM((2, NC, 3, RH, D), BF),
        pltpu.VMEM((HS, 4 * TK, 2 * D), BF),
        pltpu.VMEM((HS, 2 * TK, D), BF),
        pltpu.VMEM((NC, 2, RH, D), BF),
        pltpu.VMEM((NC, RH, D), BF),
        pltpu.VMEM((NC, R, D), BF),
        pltpu.VMEM((2, NC, R, D), BF),
        pltpu.VMEM((G, SR, D), BF),
        pltpu.VMEM((G, KR, D), BF),
        pltpu.VMEM((G, KR, D), BF),
        pltpu.VMEM((max(2, 2) * HP, max(4 * TK, 8 * CR), max(4 * TK, WIN)), BF),
        pltpu.VMEM((HP, 2 * CR, WIN), F32),
        pltpu.VMEM((R, D), BF),
        pltpu.VMEM((R, D), BF),
        pltpu.VMEM((R, FF), BF),
        pltpu.VMEM((3 * D, D), BF),
        pltpu.VMEM((D, D), BF),
        pltpu.VMEM((L, 3 * D, D), BF),
        pltpu.VMEM((D, D), BF),
        pltpu.VMEM((D, FF), BF),
        pltpu.VMEM((FF, D), BF),
        pltpu.SemaphoreType.DMA((NC, 3)),
        pltpu.SemaphoreType.DMA((2, NC, 3)),
        pltpu.SemaphoreType.DMA((NC,)),
        pltpu.SemaphoreType.DMA((NC,)),
        pltpu.SemaphoreType.DMA((NC,)),
        pltpu.SemaphoreType.DMA((2, NC)),
        pltpu.SemaphoreType.DMA((5 + L,)),
        pltpu.SemaphoreType.DMA((2,)),
        pltpu.SemaphoreType.REGULAR,
    ]
    inner = pl.BlockSpec(memory_space=pltpu.VMEM)
    outer = pl.BlockSpec(memory_space=pl.ANY)
    return pl.pallas_call(
        functools.partial(kernel, cfg),
        out_shape=(jax.ShapeDtypeStruct((NC, R, LANES), F32), jax.ShapeDtypeStruct((S, TK, LANES), F32)),
        in_specs=[pl.BlockSpec(memory_space=pltpu.SMEM)] + [inner] * 4 + [outer] * 8,
        out_specs=(inner, inner),
        scratch_shapes=scr,
        compiler_params=pltpu.CompilerParams(collective_id=0, has_side_effects=True, vmem_limit_bytes=vmem),
        name="fifo_denoise",
    )(*args)


def solution(mesh):
    MT, MF = mesh.shape["tokens"], mesh.shape["frames"]
    slot_spec = P(("videos", "frames"), "tokens", None)
    mod_spec = P(("videos", "frames"), None, None, None)
    step_spec = P(("videos", "frames"))
    noise_spec = P("videos", "tokens", None)
    emit_spec = P("videos", ("tokens", "frames"), None)
    to_sib = [(f, f ^ 1) for f in range(MF)]
    to_next_chip = [(f, (f + 2) % MF) for f in range(MF)]

    def seat(blk, q):
        here = [t for t in range(MT) if (t // 2 + blk // 2) % 2 == blk % 2 and ((t + 1) // 2) % 2 == q // 2]
        return here[0] * MF + 2 * (blk // 2) + q % 2

    places = [(blk, q) for blk in range(MF) for q in range(MT)]
    to_seat = [(q * MF + blk, seat(blk, q)) for blk, q in places]
    to_home = [(seat(blk, q), q * MF + blk) for blk, q in places]
    to_home_before = [(seat(blk, q), q * MF + (blk - 1) % MF) for blk, q in places]

    def body(z_loc, mod_loc, step_loc, noise_loc, lag_bias, w_in, w_out, w_sqkv, w_so, w_tqkv, w_to, w_up, w_down):
        SL, TK, C = z_loc.shape
        S = noise_loc.shape[0]
        L, D, FF = w_up.shape
        HD = w_so.shape[2]
        NC = CHUNKS
        CH = SL // NC
        WIN = 2 * SL * SUB
        tok, frm, chip, core, odd, half = roles(MT, MF)
        both = ("tokens", "frames")
        zn = jnp.concatenate([z_loc.reshape(SL, TK * C), noise_loc.reshape(S, TK * C)], axis=0)
        zn = lax.ppermute(zn, both, to_seat)
        z_own = zn[:SL].reshape(SL, TK, C)
        noise = zn[SL:].reshape(S, TK, C)
        pad = lambda v: jnp.pad(v, ((0, 0),) * (v.ndim - 1) + ((0, LANES - C),))

        table = jnp.concatenate([jnp.swapaxes(mod_loc, 1, 2).reshape(SL, 6 * L, D), jnp.broadcast_to(step_loc[:, None, None], (SL, 1, D))], axis=1)
        table_sib = lax.ppermute(table, "frames", to_sib)
        even_blk = jnp.where(core == 0, table, table_sib)
        odd_blk = jnp.where(core == 1, table, table_sib)
        tail = lax.ppermute(odd_blk[SL - (S - 1):], "frames", to_next_chip)
        own_tab = jnp.where(odd == 0, even_blk, odd_blk)
        prev_tab = jnp.where(odd == 0, tail, even_blk[SL - (S - 1):])

        by_output = lambda w: jnp.transpose(w, (0, 2, 3, 4, 1)).reshape(L, 3 * D, D)
        cfg = (L, S, NC, CH, TK, D, FF, HD, MT, MF, WIN)
        z_new, emit = denoise_call(
            cfg, 67043328,
            lag_bias.reshape(L * lag_bias.shape[1], -1), pad(z_own).reshape(NC, CH * TK, LANES), pad(noise),
            jnp.pad(w_in, ((0, LANES - C), (0, 0))), jnp.pad(w_out, ((0, 0), (0, LANES - C))), own_tab, prev_tab,
            by_output(w_sqkv), w_so.reshape(L, D, D), by_output(w_tqkv), w_to.reshape(L, D, D), w_up, w_down,
        )

        mine = jnp.concatenate([z_new.reshape(SL, TK, LANES)[:, :, :C].reshape(SL, TK * C), emit[:, :, :C].reshape(S, TK * C)], axis=0)
        late = lax.ppermute(mine[S:], both, to_home)
        early = lax.ppermute(mine[:S], both, to_home_before)
        z_fin = jnp.concatenate([late[:SL - S], early], axis=0).reshape(SL, TK, C)
        per = TK // MF
        em = jnp.swapaxes(late[SL - S:].reshape(S, MF, per * C), 0, 1)
        em = lax.all_to_all(em, "frames", 0, 0, tiled=True)[0].reshape(S, per, C)
        return em, z_fin

    return jax.shard_map(body, mesh=mesh, in_specs=(slot_spec, mod_spec, step_spec, noise_spec) + (P(),) * 9, out_specs=(emit_spec, slot_spec), check_vma=False)
```

```python
import functools

import jax
import jax.numpy as jnp
from jax import lax
from jax.experimental import pallas as pl
from jax.experimental.pallas import tpu as pltpu
from jax.sharding import PartitionSpec as P

MESH = pl.DeviceIdType.MESH
BF = jnp.bfloat16
F32 = jnp.float32
LANES = 128
SUB = 8
CHUNKS = 4


def mm(a, b):
    return jnp.dot(a, b, preferred_element_type=F32)


def mm_t(a, b):
    return lax.dot_general(a, b, (((1,), (1,)), ((), ())), preferred_element_type=F32)


def norm(xv):
    mean = jnp.mean(xv, axis=-1, keepdims=True)
    cen = xv - mean
    var = jnp.mean(cen * cen, axis=-1, keepdims=True)
    return cen * lax.rsqrt(var + 1e-6)


def gelu(hv):
    inner = 0.7978845608028654 * (hv + 0.044715 * (hv * hv * hv))
    return 0.5 * hv * (1.0 + jnp.tanh(inner))


def roles(mesh_tokens, mesh_frames):
    tok, frm = lax.axis_index("tokens"), lax.axis_index("frames")
    chip, core = frm // 2, frm % 2
    odd = (tok // 2 + chip) % 2
    half = ((tok + 1) // 2) % 2
    return tok, frm, chip, core, odd, half


def kernel(cfg, lag_bias, z_in, z_near, noise, w_in, w_out, own_tab, prev_tab, sqkv_h, so_h, tqkv_h, to_h, up_h, down_h, z, emit,
           mod, bias, x, ust, us, kvs, qs, obuf, osnd, ut, utr, qt, kt, vt, pb, bm, ob, uu, hb,
           sqkv, so, tqkv, to, up, down,
           us_s, us_r, o_s, o_r, ut_s, ut_r, w_sem, t_sem, credit):
    L, S, NC, CH, TK, D, FF, HD, MT, MF, WIN = cfg
    R, HS, RH, G = CH * TK, CH // 2, CH * TK // 2, TK // SUB
    CR = CH * SUB
    SR = NC * CH * SUB
    NT = L * S
    HP = D // LANES
    W = min(256, D)
    DT = D // W
    FT = min(256, FF)
    qscale = HD ** -0.5
    SU, TU, RS = min(2, HS), min(8, G), min(64, 4 * TK)

    vid = lax.axis_index("videos")
    tok, frm, chip, core, odd, _ = roles(MT, MF)
    sib_f = frm + 1 - 2 * core
    par_t = tok + 1 - 2 * (tok % 2)
    block = chip * 2 + odd
    first = block == 0
    sib = (vid, tok, sib_f)
    par_a = (vid, par_t, frm)
    par_b = (vid, par_t, sib_f)
    nxt = (vid, jnp.where(odd == 0, MT - 1 - tok, tok), jnp.where(odd == 0, frm, (frm + 2) % MF))
    prv = (vid, jnp.where(odd == 1, MT - 1 - tok, tok), jnp.where(odd == 1, frm, (frm + MF - 2) % MF))

    def w_copy(k, layer):
        src, dst = ((sqkv_h, sqkv), (so_h, so), (to_h, to), (up_h, up), (down_h, down))[k]
        return pltpu.make_async_copy(src.at[layer], dst, w_sem.at[k])

    def t_copy(layer):
        return pltpu.make_async_copy(tqkv_h.at[layer], tqkv.at[layer], w_sem.at[5 + layer])

    tables = (
        pltpu.make_async_copy(prev_tab, mod.at[0:S - 1], t_sem.at[0]),
        pltpu.make_async_copy(own_tab, mod.at[S - 1:S - 1 + NC * CH], t_sem.at[1]),
    )
    for c in tables:
        c.start()
    w_copy(0, 0).start()
    w_copy(1, 0).start()
    for layer in range(L):
        t_copy(layer).start()

    barrier = pltpu.get_barrier_semaphore()
    for dev in (sib, par_a, par_b, nxt, prv):
        pl.semaphore_signal(barrier, inc=1, device_id=dev, device_id_type=MESH)
    pl.semaphore_wait(barrier, 5)

    def remote(src, dst, ss, rs, dev):
        return pltpu.make_async_remote_copy(src_ref=src, dst_ref=dst, send_sem=ss, recv_sem=rs, device_id=dev, device_id_type=MESH)

    def us_copies(par, i):
        return (
            remote(ust.at[i, 1 - core], us.at[par, i, 0], us_s.at[i, 0], us_r.at[par, i, 0], sib),
            remote(ust.at[i, core], us.at[par, i, 1], us_s.at[i, 1], us_r.at[par, i, 1], par_a),
            remote(ust.at[i, 1 - core], us.at[par, i, 2], us_s.at[i, 2], us_r.at[par, i, 2], par_b),
        )

    def o_copy(i):
        return remote(osnd.at[i], obuf.at[i, core], o_s.at[i], o_r.at[i], sib)

    unread = TK * max(0, min(NC * CH + 1 - lag_bias.shape[1], CH - 1))

    def ut_each(par, i, act):
        def part(row):
            act(remote(ut.at[i, row:R], utr.at[par, i, row:R], ut_s.at[i], ut_r.at[par, i], nxt))

        pl.when(i == 0)(lambda: part(unread))
        pl.when(i > 0)(lambda: part(0))

    z[...] = z_in[...]
    emit[...] = jnp.zeros_like(emit)
    if unread:
        utr[:, 0, 0:unread, :] = jnp.zeros((2, unread, D), BF)
    for g in range(G):
        for ref in (kt, vt):
            ref[g] = jnp.zeros(ref.shape[1:], BF)

    q_row = lax.broadcasted_iota(jnp.int32, (CR, WIN), 0)
    k_col = lax.broadcasted_iota(jnp.int32, (CR, WIN), 1)
    lag = NC * CH + q_row // SUB - k_col // SUB
    lag = jnp.where((q_row & (SUB - 1)) == (k_col & (SUB - 1)), lag, -1)

    @pl.loop(0, L * HP)
    def _(lh):
        for hd in range(2):
            tile = jnp.full((CR, WIN), -jnp.inf, F32)
            for r in range(lag_bias.shape[1]):
                tile = jnp.where(lag == r, lag_bias[2 * lh + hd, r], tile)
            bias[lh // HP, lh % HP, hd * CR:(hd + 1) * CR, :] = tile

    for c in tables:
        c.wait()

    lane = lax.broadcasted_iota(jnp.int32, (1, LANES), 1)
    low = lane < HD

    def stack_heads(q):
        zero = jnp.zeros_like(q)
        return jnp.concatenate([jnp.where(low, q, zero), jnp.where(low, zero, q)], axis=0)

    def softmax_rows(sv):
        top = jnp.max(sv, axis=-1, keepdims=True)
        e = jnp.exp(sv - top)
        return (e * (1.0 / jnp.sum(e, axis=-1, keepdims=True))).astype(BF)

    NR = min(32, TK)

    def affine(slot, layer, step, which):
        row = slot + (S - 1) - step
        return 1.0 + mod[row, pl.ds((2 * which + 1) * L + layer, 1), :], mod[row, pl.ds(2 * which * L + layer, 1), :]

    def modulated(i, a, layer, step, which, put):
        gain, shift = affine(i * CH + a, layer, step, which)
        for r in range(0, TK, NR):
            xv = x[i, a * TK + r:a * TK + r + NR, :]
            put(r, (norm(xv) * gain + shift).astype(BF))

    def spatial(i, par, n):
        @pl.when(n > 0)
        def _():
            for c in us_copies(par, i):
                c.wait()

        own = ust[i, core]
        u_all = jnp.concatenate([own, us[par, i, 0], us[par, i, 1], us[par, i, 2]], axis=0)
        u_q = jnp.concatenate([own, us[par, i, 0]], axis=0)
        for t in range(DT):
            y = (mm_t(u_q, sqkv[t * W:(t + 1) * W, :]) * qscale).astype(BF)
            for p in range(2):
                for s in range(HS):
                    qs[s, p * TK:(p + 1) * TK, t * W:(t + 1) * W] = y[p * RH + s * TK:p * RH + (s + 1) * TK]
        for t in range(2 * DT):
            y = mm_t(u_all, sqkv[D + t * W:D + (t + 1) * W, :]).astype(BF)
            for p in range(4):
                for s in range(HS):
                    kvs[s, p * TK:(p + 1) * TK, t * W:(t + 1) * W] = y[p * RH + s * TK:p * RH + (s + 1) * TK]

        @pl.loop(0, HS // SU)
        def _(ss):
            units = [(ss * SU + d, d * HP + h, h) for d in range(SU) for h in range(HP)]
            for s, p, h in units:
                cols = slice(h * LANES, (h + 1) * LANES)
                sv = mm_t(stack_heads(qs[s, :, cols]), kvs[s, :, cols])
                for r in range(0, 4 * TK, RS):
                    pb[p, r:r + RS, 0:4 * TK] = softmax_rows(sv[r:r + RS])
            for s, p, h in units:
                cols = slice(h * LANES, (h + 1) * LANES)
                o2 = mm(pb[p, 0:4 * TK, 0:4 * TK], kvs[s, :, D + h * LANES:D + (h + 1) * LANES])
                o = jnp.where(low, o2[:2 * TK], o2[2 * TK:]).astype(BF)
                rows = pl.ds(pl.multiple_of(s * TK, TK), TK)
                obuf[i, core, rows, cols] = o[:TK]
                osnd[i, rows, cols] = o[TK:]

        o_copy(i).start()

    def project(i, par, layer, step, n):
        o_copy(i).wait()
        ov = obuf[i].reshape(R, D)
        for r in range(0, R, R // 2):
            for t in range(DT):
                cols = slice(t * W, (t + 1) * W)
                x[i, r:r + R // 2, cols] = x[i, r:r + R // 2, cols] + mm(ov[r:r + R // 2], so[:, cols])
        for a in range(CH):
            def put(r, v, a=a):
                ut[i, a * TK + r:a * TK + r + NR, :] = v

            modulated(i, a, layer, step, 1, put)

        @pl.when((i == NC - 1) & (n >= 2))
        def _():
            pl.semaphore_wait(credit, 1)

        ut_each(par, i, lambda c: c.start())

    def own_qkv(i, layer):
        uv = ut[i]
        for t in range(3 * DT):
            y = mm_t(uv, tqkv[layer, t * W:(t + 1) * W, :])
            kind, tt = t // DT, t % DT
            if kind == 0:
                y = y * qscale
            y4 = y.reshape(CH, G, SUB, W)
            for g in range(G):
                yg = y4[:, g].reshape(CR, W).astype(BF)
                if kind == 0:
                    qt[g, pl.ds(pl.multiple_of(i * CR, CR), CR), tt * W:(tt + 1) * W] = yg
                else:
                    ref = kt if kind == 1 else vt
                    ref[g, pl.ds(pl.multiple_of(SR + i * CR, CR), CR), tt * W:(tt + 1) * W] = yg

    def temporal(i, par, layer, step):
        ut_each(par, i, lambda c: c.wait())
        uv = utr[par, i]
        for t in range(2 * DT):
            y = mm_t(uv, tqkv[layer, D + t * W:D + (t + 1) * W, :])
            kind, tt = t // DT, t % DT
            ref = vt if kind else kt
            y4 = y.reshape(CH, G, SUB, W)
            for g in range(G):
                ref[g, pl.ds(pl.multiple_of(i * CR, CR), CR), tt * W:(tt + 1) * W] = y4[:, g].reshape(CR, W).astype(BF)
        rows = lax.broadcasted_iota(jnp.int32, (2 * CR, WIN), 0)
        keys = lax.broadcasted_iota(jnp.int32, (2 * CR, WIN), 1)
        pos_q = i * CH + (rows & (CR - 1)) // SUB
        pos_k = (i - NC) * CH + keys // SUB
        pos = block * NC * CH + pos_q - step
        slot = jnp.where(pos < 0, pos + MF * NC * CH, pos)
        valid = pos_q - pos_k <= slot
        for h in range(HP):
            bm[h] = jnp.where(valid, bias[layer, h], -jnp.inf)

        @pl.loop(0, G // TU)
        def _(gg):
            qrows = pl.ds(pl.multiple_of(i * CR, CR), CR)
            krows = pl.ds(pl.multiple_of(i * CR, CR), WIN)
            units = [(gg * TU + d, d * 2 * CR, h) for d in range(TU) for h in range(HP)]
            for g, r, h in units:
                cols = slice(h * LANES, (h + 1) * LANES)
                sv = mm_t(stack_heads(qt[g, qrows, cols]), kt[g, krows, cols]) + bm[h]
                pb[h, r:r + 2 * CR, 0:WIN] = softmax_rows(sv)
            for g, r, h in units:
                cols = slice(h * LANES, (h + 1) * LANES)
                o2 = mm(pb[h, r:r + 2 * CR, 0:WIN], vt[g, krows, cols])
                ob[pl.ds(pl.multiple_of(g * CR, CR), CR), cols] = jnp.where(low, o2[:CR], o2[CR:]).astype(BF)

        ov = ob[...]
        for r in range(0, R, R // 2):
            for t in range(DT):
                cols = slice(t * W, (t + 1) * W)
                r0, r1 = r, r + R // 2
                g0, gn = r0 // CR, (r1 - r0) // CR
                y4 = mm(ov[r0:r1], to[:, cols]).reshape(gn, CH, SUB, W)
                for a in range(CH):
                    rows = slice(a * TK + g0 * SUB, a * TK + (g0 + gn) * SUB)
                    x[i, rows, cols] = x[i, rows, cols] + y4[:, a].reshape(gn * SUB, W)

    def mlp(i, layer, step):
        for a in range(CH):
            def put(r, v, a=a):
                uu[a * TK + r:a * TK + r + NR, :] = v

            modulated(i, a, layer, step, 2, put)
        uv = uu[...]
        for t in range(FF // FT):
            hp = mm(uv, up[:, t * FT:(t + 1) * FT])
            for r in range(0, R, min(R, 128)):
                hb[r:r + 128, t * FT:(t + 1) * FT] = gelu(hp[r:r + 128]).astype(BF)
        for r in range(0, R, R // 2):
            for t in range(DT):
                cols = slice(t * W, (t + 1) * W)
                x[i, r:r + R // 2, cols] = x[i, r:r + R // 2, cols] + mm(hb[r:r + R // 2], down[:, cols])

    def embed(zv):
        return mm(zv.astype(BF), w_in[...]).astype(BF).astype(F32)

    def ready(i, layer, step):
        for a in range(CH):
            def put(r, v, a=a):
                ust[i, a // HS, (a % HS) * TK + r:(a % HS) * TK + r + NR, :] = v

            modulated(i, a, layer, step, 0, put)

    def turn(i, step):
        for r in range(0, R, RH):
            for q in range(r, r + RH, NR):
                uu[q:q + NR, :] = norm(x[i, q:q + NR, :]).astype(BF)
            v = mm(uu[r:r + RH], w_out[...])
            entering = []
            for a in range(r // TK, (r + RH) // TK):
                dt = mod[i * CH + a + (S - 1) - step, pl.ds(6 * L, 1), 0:LANES]
                zv = z[i, a * TK:(a + 1) * TK, :] + dt * v[a * TK - r:(a + 1) * TK - r]
                z[i, a * TK:(a + 1) * TK, :] = zv
                entering.append(jnp.where(first & (i * CH + a == step), noise[step], zv))
            x[i, r:r + RH, :] = embed(jnp.concatenate(entering, axis=0))

    def replace_head(step):
        rows = pl.ds(pl.multiple_of((step % CH) * TK, TK), TK)
        zv = z[step // CH, rows, :]
        emit[step] = zv
        z[step // CH, rows, :] = jnp.where(first, noise[step], zv)

    def begin(i):
        x[i] = embed(z[i])
        ready(i, 0, 0)
        mine = pl.ds(pl.multiple_of(core * RH, RH), RH)
        for k in range(3):
            xv = embed(z_near[k, i, mine, :])
            for s in range(HS):
                gain, shift = affine(i * CH + core * HS + s, 0, 0, 0)
                us[0, i, k, s * TK:(s + 1) * TK, :] = (norm(xv[s * TK:(s + 1) * TK]) * gain + shift).astype(BF)

    @pl.loop(0, NT + 1)
    def _(m):
        n = m - 1
        layer, step, par = lax.rem(n + L, L), (n + L) // L - 1, lax.rem(n + 2, 2)
        nlayer, nstep, npar = lax.rem(m, L), m // L, lax.rem(m, 2)

        @pl.when(m > 0)
        def _():
            w_copy(0, layer).wait()
            w_copy(1, layer).wait()

            @pl.when(m == 1)
            def _():
                for q in range(L):
                    t_copy(q).wait()

            for k in (2, 3, 4):
                w_copy(k, layer).start()

            @pl.loop(0, NC + 1)
            def _(c):
                @pl.when(c < NC)
                def _():
                    spatial(NC - 1 - c, par, n)

                @pl.when(c > 0)
                def _():
                    own_qkv(NC - c, layer)

                @pl.when(c < NC)
                def _():
                    project(NC - 1 - c, par, layer, step, n)

            for k in (2, 3, 4):
                w_copy(k, layer).wait()

            @pl.when(m < NT)
            def _():
                w_copy(0, nlayer).start()
                w_copy(1, nlayer).start()

        @pl.loop(0, NC)
        def _(c):
            i = NC - 1 - c

            @pl.when(m == 0)
            def _():
                begin(i)

            @pl.when(m > 0)
            def _():
                temporal(i, par, layer, step)
                mlp(i, layer, step)
                ready(i, nlayer, jnp.minimum(nstep, S - 1))

                @pl.when(layer == L - 1)
                def _():
                    turn(i, step)
                    ready(i, nlayer, jnp.minimum(nstep, S - 1))

                @pl.when(m < NT)
                def _():
                    for c in us_copies(npar, i):
                        c.start()

        @pl.when((m > 0) & (layer == L - 1))
        def _():
            replace_head(step)

        @pl.when(m > 0)
        def _():
            pl.semaphore_signal(credit, inc=1, device_id=prv, device_id_type=MESH)

    pl.semaphore_wait(credit, min(2, NT))


def denoise_call(cfg, vmem, *args):
    L, S, NC, CH, TK, D, FF, HD, MT, MF, WIN = cfg
    R, HS, RH, G = CH * TK, CH // 2, CH * TK // 2, TK // SUB
    CR, SR = CH * SUB, NC * CH * SUB
    HP = D // LANES
    KR = (NC - 1) * CR + WIN
    scr = [
        pltpu.VMEM((S - 1 + NC * CH, 6 * L + 1, D), F32),
        pltpu.VMEM((L, HP, 2 * CR, WIN), F32),
        pltpu.VMEM((NC, R, D), F32),
        pltpu.VMEM((NC, 2, RH, D), BF),
        pltpu.VMEM((2, NC, 3, RH, D), BF),
        pltpu.VMEM((HS, 4 * TK, 2 * D), BF),
        pltpu.VMEM((HS, 2 * TK, D), BF),
        pltpu.VMEM((NC, 2, RH, D), BF),
        pltpu.VMEM((NC, RH, D), BF),
        pltpu.VMEM((NC, R, D), BF),
        pltpu.VMEM((2, NC, R, D), BF),
        pltpu.VMEM((G, SR, D), BF),
        pltpu.VMEM((G, KR, D), BF),
        pltpu.VMEM((G, KR, D), BF),
        pltpu.VMEM((max(2, 2) * HP, max(4 * TK, 16 * CR), max(4 * TK, WIN)), BF),
        pltpu.VMEM((HP, 2 * CR, WIN), F32),
        pltpu.VMEM((R, D), BF),
        pltpu.VMEM((R, D), BF),
        pltpu.VMEM((R, FF), BF),
        pltpu.VMEM((3 * D, D), BF),
        pltpu.VMEM((D, D), BF),
        pltpu.VMEM((L, 3 * D, D), BF),
        pltpu.VMEM((D, D), BF),
        pltpu.VMEM((D, FF), BF),
        pltpu.VMEM((FF, D), BF),
        pltpu.SemaphoreType.DMA((NC, 3)),
        pltpu.SemaphoreType.DMA((2, NC, 3)),
        pltpu.SemaphoreType.DMA((NC,)),
        pltpu.SemaphoreType.DMA((NC,)),
        pltpu.SemaphoreType.DMA((NC,)),
        pltpu.SemaphoreType.DMA((2, NC)),
        pltpu.SemaphoreType.DMA((5 + L,)),
        pltpu.SemaphoreType.DMA((2,)),
        pltpu.SemaphoreType.REGULAR,
    ]
    inner = pl.BlockSpec(memory_space=pltpu.VMEM)
    outer = pl.BlockSpec(memory_space=pl.ANY)
    return pl.pallas_call(
        functools.partial(kernel, cfg),
        out_shape=(jax.ShapeDtypeStruct((NC, R, LANES), F32), jax.ShapeDtypeStruct((S, TK, LANES), F32)),
        in_specs=[pl.BlockSpec(memory_space=pltpu.SMEM)] + [inner] * 5 + [outer] * 8,
        out_specs=(inner, inner),
        scratch_shapes=scr,
        compiler_params=pltpu.CompilerParams(collective_id=0, has_side_effects=True, vmem_limit_bytes=vmem),
        name="fifo_denoise",
    )(*args)


def solution(mesh):
    MT, MF = mesh.shape["tokens"], mesh.shape["frames"]
    slot_spec = P(("videos", "frames"), "tokens", None)
    mod_spec = P(("videos", "frames"), None, None, None)
    step_spec = P(("videos", "frames"))
    noise_spec = P("videos", "tokens", None)
    emit_spec = P("videos", ("tokens", "frames"), None)
    to_sib = [(f, f ^ 1) for f in range(MF)]
    to_next_chip = [(f, (f + 2) % MF) for f in range(MF)]

    def seat(blk, q):
        here = [t for t in range(MT) if (t // 2 + blk // 2) % 2 == blk % 2 and ((t + 1) // 2) % 2 == q // 2]
        return here[0] * MF + 2 * (blk // 2) + q % 2

    places = [(blk, q) for blk in range(MF) for q in range(MT)]
    to_seat = [(q * MF + blk, seat(blk, q)) for blk, q in places]
    to_near = [[((q ^ k) * MF + blk, seat(blk, q)) for blk, q in places] for k in (1, 2, 3)]
    to_home = [(seat(blk, q), q * MF + blk) for blk, q in places]
    to_home_before = [(seat(blk, q), q * MF + (blk - 1) % MF) for blk, q in places]

    def body(z_loc, mod_loc, step_loc, noise_loc, lag_bias, w_in, w_out, w_sqkv, w_so, w_tqkv, w_to, w_up, w_down):
        SL, TK, C = z_loc.shape
        S = noise_loc.shape[0]
        L, D, FF = w_up.shape
        HD = w_so.shape[2]
        NC = CHUNKS
        CH = SL // NC
        WIN = 2 * SL * SUB
        tok, frm, chip, core, odd, half = roles(MT, MF)
        both = ("tokens", "frames")
        zn = jnp.concatenate([z_loc.reshape(SL, TK * C), noise_loc.reshape(S, TK * C)], axis=0)
        zn = lax.ppermute(zn, both, to_seat)
        z_all = jnp.concatenate([zn[:SL]] + [lax.ppermute(z_loc.reshape(SL, TK * C), both, p) for p in to_near], axis=0).reshape(4, SL, TK, C)
        noise = zn[SL:].reshape(S, TK, C)
        pad = lambda v: jnp.pad(v, ((0, 0),) * (v.ndim - 1) + ((0, LANES - C),))

        table = jnp.concatenate([jnp.swapaxes(mod_loc, 1, 2).reshape(SL, 6 * L, D), jnp.broadcast_to(step_loc[:, None, None], (SL, 1, D))], axis=1)
        table_sib = lax.ppermute(table, "frames", to_sib)
        even_blk = jnp.where(core == 0, table, table_sib)
        odd_blk = jnp.where(core == 1, table, table_sib)
        tail = lax.ppermute(odd_blk[SL - (S - 1):], "frames", to_next_chip)
        own_tab = jnp.where(odd == 0, even_blk, odd_blk)
        prev_tab = jnp.where(odd == 0, tail, even_blk[SL - (S - 1):])

        by_output = lambda w: jnp.transpose(w, (0, 2, 3, 4, 1)).reshape(L, 3 * D, D)
        z_tiles = pad(z_all).reshape(4, NC, CH * TK, LANES)
        cfg = (L, S, NC, CH, TK, D, FF, HD, MT, MF, WIN)
        z_new, emit = denoise_call(
            cfg, 67043328,
            lag_bias.reshape(L * lag_bias.shape[1], -1), z_tiles[0], z_tiles[1:], pad(noise),
            jnp.pad(w_in, ((0, LANES - C), (0, 0))), jnp.pad(w_out, ((0, 0), (0, LANES - C))), own_tab, prev_tab,
            by_output(w_sqkv), w_so.reshape(L, D, D), by_output(w_tqkv), w_to.reshape(L, D, D), w_up, w_down,
        )

        mine = jnp.concatenate([z_new.reshape(SL, TK, LANES)[:, :, :C].reshape(SL, TK * C), emit[:, :, :C].reshape(S, TK * C)], axis=0)
        late = lax.ppermute(mine[S:], both, to_home)
        early = lax.ppermute(mine[:S], both, to_home_before)
        z_fin = jnp.concatenate([late[:SL - S], early], axis=0).reshape(SL, TK, C)
        per = TK // MF
        em = jnp.swapaxes(late[SL - S:].reshape(S, MF, per * C), 0, 1)
        em = lax.all_to_all(em, "frames", 0, 0, tiled=True)[0].reshape(S, per, C)
        return em, z_fin

    return jax.shard_map(body, mesh=mesh, in_specs=(slot_spec, mod_spec, step_spec, noise_spec) + (P(),) * 9, out_specs=(emit_spec, slot_spec), check_vma=False)
```

```python
import functools

import jax
import jax.numpy as jnp
from jax import lax
from jax.experimental import pallas as pl
from jax.experimental.pallas import tpu as pltpu
from jax.sharding import PartitionSpec as P

MESH = pl.DeviceIdType.MESH
BF = jnp.bfloat16
F32 = jnp.float32
LANES = 128
CPAD = 16
SUB = 8
CHUNKS = 4


def mm(a, b):
    return jnp.dot(a, b, preferred_element_type=F32)


def mm_t(a, b):
    return lax.dot_general(a, b, (((1,), (1,)), ((), ())), preferred_element_type=F32)


def tt_mm(a, b):
    return lax.dot_general(a, b, (((0,), (0,)), ((), ())), preferred_element_type=F32)


def norm(xv):
    mean = jnp.mean(xv, axis=-1, keepdims=True)
    cen = xv - mean
    var = jnp.mean(cen * cen, axis=-1, keepdims=True)
    return cen * lax.rsqrt(var + 1e-6)


def gelu(hv):
    inner = 0.7978845608028654 * (hv + 0.044715 * (hv * hv * hv))
    return 0.5 * hv * (1.0 + jnp.tanh(inner))


def roles(mesh_tokens, mesh_frames):
    tok, frm = lax.axis_index("tokens"), lax.axis_index("frames")
    chip, core = frm // 2, frm % 2
    odd = (tok // 2 + chip) % 2
    half = ((tok + 1) // 2) % 2
    return tok, frm, chip, core, odd, half


def kernel(cfg, lag_bias, z_mine, w_in, w_out, own_tab, prev_tab, sqkv_h, so_h, tqkv_h, to_h, up_h, down_h, late, early,
           mod, bias, z, zq, nz, wi, wo, x, ust, us, kvs, qs, obuf, osnd, ut, utr, qt, kt, vt, pb, bm, ob, uu, hb,
           sqkv, so, tqkv, to, up, down,
           us_s, us_r, o_s, o_r, ut_s, ut_r, w_sem, t_sem, z_s, z_r, credit):
    L, S, NC, CH, TK, D, FF, HD, MT, MF, WIN = cfg
    R, HS, RH, G = CH * TK, CH // 2, CH * TK // 2, TK // SUB
    CR = CH * SUB
    SR = NC * CH * SUB
    NT = L * S
    HP = D // LANES
    W = min(256, D)
    DT = D // W
    FT = min(256, FF)
    qscale = HD ** -0.5
    NCH = w_in.shape[0]
    SU, TU, RS = min(2, HS), min(8, G), min(64, 4 * TK)

    vid = lax.axis_index("videos")
    tok, frm, chip, core, odd, _ = roles(MT, MF)
    sib_f = frm + 1 - 2 * core
    par_t = tok + 1 - 2 * (tok % 2)
    block = chip * 2 + odd
    first = block == 0
    sib = (vid, tok, sib_f)
    par_a = (vid, par_t, frm)
    par_b = (vid, par_t, sib_f)
    nxt = (vid, jnp.where(odd == 0, MT - 1 - tok, tok), jnp.where(odd == 0, frm, (frm + 2) % MF))
    prv = (vid, jnp.where(odd == 1, MT - 1 - tok, tok), jnp.where(odd == 1, frm, (frm + MF - 2) % MF))

    def w_copy(k, layer):
        src, dst = ((sqkv_h, sqkv), (so_h, so), (to_h, to), (up_h, up), (down_h, down))[k]
        return pltpu.make_async_copy(src.at[layer], dst, w_sem.at[k])

    def t_copy(layer):
        return pltpu.make_async_copy(tqkv_h.at[layer], tqkv.at[layer], w_sem.at[5 + layer])

    tables = (
        pltpu.make_async_copy(prev_tab, mod.at[0:S - 1], t_sem.at[0]),
        pltpu.make_async_copy(own_tab, mod.at[S - 1:S - 1 + NC * CH], t_sem.at[1]),
    )
    for c in tables:
        c.start()
    w_copy(0, 0).start()
    w_copy(1, 0).start()
    for layer in range(L):
        t_copy(layer).start()

    wi[...] = jnp.zeros_like(wi)
    wo[...] = jnp.zeros_like(wo)
    wi[0:NCH] = w_in[...]
    wo[0:NCH] = w_out[...]
    for ref in (z, nz):
        ref[...] = jnp.zeros_like(ref)
    for k in range(NC * CH):
        i, lanes = k // CH, slice(k % CH * TK, (k % CH + 1) * TK)
        z[i, 0:NCH, lanes] = z_mine[k]
    for k in range(S):
        for a in range(CH):
            nz[k, 0:NCH, a * TK:(a + 1) * TK] = z_mine[NC * CH + k]
    barrier = pltpu.get_barrier_semaphore()
    for dev in (sib, par_a, par_b, nxt, prv):
        pl.semaphore_signal(barrier, inc=1, device_id=dev, device_id_type=MESH)
    pl.semaphore_wait(barrier, 5)

    def remote(src, dst, ss, rs, dev):
        return pltpu.make_async_remote_copy(src_ref=src, dst_ref=dst, send_sem=ss, recv_sem=rs, device_id=dev, device_id_type=MESH)

    def us_copies(par, i):
        return (
            remote(ust.at[i, 1 - core], us.at[par, i, 0], us_s.at[i, 0], us_r.at[par, i, 0], sib),
            remote(ust.at[i, core], us.at[par, i, 1], us_s.at[i, 1], us_r.at[par, i, 1], par_a),
            remote(ust.at[i, 1 - core], us.at[par, i, 2], us_s.at[i, 2], us_r.at[par, i, 2], par_b),
        )

    def o_copy(i):
        return remote(osnd.at[i], obuf.at[i, core], o_s.at[i], o_r.at[i], sib)

    unread = TK * max(0, min(NC * CH + 1 - lag_bias.shape[1], CH - 1))

    def ut_each(par, i, act):
        def part(row):
            act(remote(ut.at[i, row:R], utr.at[par, i, row:R], ut_s.at[i], ut_r.at[par, i], nxt))

        if isinstance(i, int):
            part(unread if i == 0 else 0)
        else:
            pl.when(i == 0)(lambda: part(unread))
            pl.when(i > 0)(lambda: part(0))

    near = [remote(z, zq.at[k], z_s.at[k], z_r.at[k], dev) for k, dev in enumerate((sib, par_a, par_b))]
    for c in near:
        c.start()
    if unread:
        utr[:, 0, 0:unread, :] = jnp.zeros((2, unread, D), BF)
    for g in range(G):
        for ref in (kt, vt):
            ref[g] = jnp.zeros(ref.shape[1:], BF)

    q_row = lax.broadcasted_iota(jnp.int32, (CR, WIN), 0)
    k_col = lax.broadcasted_iota(jnp.int32, (CR, WIN), 1)
    lag = NC * CH + q_row // SUB - k_col // SUB
    lag = jnp.where((q_row & (SUB - 1)) == (k_col & (SUB - 1)), lag, -1)

    @pl.loop(0, L * HP)
    def _(lh):
        for hd in range(2):
            tile = jnp.full((CR, WIN), -jnp.inf, F32)
            for r in range(lag_bias.shape[1]):
                tile = jnp.where(lag == r, lag_bias[2 * lh + hd, r], tile)
            bias[lh // HP, lh % HP, hd * CR:(hd + 1) * CR, :] = tile

    for c in tables:
        c.wait()
    for c in near:
        c.wait()

    lane = lax.broadcasted_iota(jnp.int32, (1, LANES), 1)
    low = lane < HD

    def stack_heads(q):
        zero = jnp.zeros_like(q)
        return jnp.concatenate([jnp.where(low, q, zero), jnp.where(low, zero, q)], axis=0)

    def softmax_rows(sv):
        top = jnp.max(sv, axis=-1, keepdims=True)
        e = jnp.exp(sv - top)
        return (e * (1.0 / jnp.sum(e, axis=-1, keepdims=True))).astype(BF)

    NR = min(32, TK)

    def affine(slot, layer, step, which):
        row = slot + (S - 1) - step
        return 1.0 + mod[row, pl.ds((2 * which + 1) * L + layer, 1), :], mod[row, pl.ds(2 * which * L + layer, 1), :]

    def modulated(i, a, layer, step, which, put):
        gain, shift = affine(i * CH + a, layer, step, which)
        for r in range(0, TK, NR):
            xv = x[i, a * TK + r:a * TK + r + NR, :]
            put(r, (norm(xv) * gain + shift).astype(BF))

    def spatial(i, par, n):
        @pl.when(n > 0)
        def _():
            for c in us_copies(par, i):
                c.wait()

        own = ust[i, core]
        u_all = jnp.concatenate([own, us[par, i, 0], us[par, i, 1], us[par, i, 2]], axis=0)
        u_q = jnp.concatenate([own, us[par, i, 0]], axis=0)
        for t in range(DT):
            y = (mm_t(u_q, sqkv[t * W:(t + 1) * W, :]) * qscale).astype(BF)
            for p in range(2):
                for s in range(HS):
                    qs[s, p * TK:(p + 1) * TK, t * W:(t + 1) * W] = y[p * RH + s * TK:p * RH + (s + 1) * TK]
        for t in range(2 * DT):
            y = mm_t(u_all, sqkv[D + t * W:D + (t + 1) * W, :]).astype(BF)
            for p in range(4):
                for s in range(HS):
                    kvs[s, p * TK:(p + 1) * TK, t * W:(t + 1) * W] = y[p * RH + s * TK:p * RH + (s + 1) * TK]

        @pl.loop(0, HS // SU)
        def _(ss):
            units = [(ss * SU + d, d * HP + h, h) for d in range(SU) for h in range(HP)]
            for s, p, h in units:
                cols = slice(h * LANES, (h + 1) * LANES)
                sv = mm_t(stack_heads(qs[s, :, cols]), kvs[s, :, cols])
                for r in range(0, 4 * TK, RS):
                    pb[p, r:r + RS, 0:4 * TK] = softmax_rows(sv[r:r + RS])
            for s, p, h in units:
                cols = slice(h * LANES, (h + 1) * LANES)
                o2 = mm(pb[p, 0:4 * TK, 0:4 * TK], kvs[s, :, D + h * LANES:D + (h + 1) * LANES])
                o = jnp.where(low, o2[:2 * TK], o2[2 * TK:]).astype(BF)
                rows = pl.ds(pl.multiple_of(s * TK, TK), TK)
                obuf[i, core, rows, cols] = o[:TK]
                osnd[i, rows, cols] = o[TK:]

        o_copy(i).start()

    def project(i, par, layer, step, n):
        o_copy(i).wait()
        ov = obuf[i].reshape(R, D)
        for r in range(0, R, R // 2):
            for t in range(DT):
                cols = slice(t * W, (t + 1) * W)
                x[i, r:r + R // 2, cols] = x[i, r:r + R // 2, cols] + mm(ov[r:r + R // 2], so[:, cols])
        for a in range(CH):
            def put(r, v, a=a):
                ut[i, a * TK + r:a * TK + r + NR, :] = v

            modulated(i, a, layer, step, 1, put)

        @pl.when((i == NC - 1) & (n >= 2))
        def _():
            pl.semaphore_wait(credit, 1)

        ut_each(par, i, lambda c: c.start())

    def own_qkv(i, layer):
        uv = ut[i]
        for t in range(3 * DT):
            y = mm_t(uv, tqkv[layer, t * W:(t + 1) * W, :])
            kind, tt = t // DT, t % DT
            if kind == 0:
                y = y * qscale
            y4 = y.reshape(CH, G, SUB, W)
            for g in range(G):
                yg = y4[:, g].reshape(CR, W).astype(BF)
                if kind == 0:
                    qt[g, pl.ds(pl.multiple_of(i * CR, CR), CR), tt * W:(tt + 1) * W] = yg
                else:
                    ref = kt if kind == 1 else vt
                    ref[g, pl.ds(pl.multiple_of(SR + i * CR, CR), CR), tt * W:(tt + 1) * W] = yg

    def halo_kv(i, par, layer):
        ut_each(par, i, lambda c: c.wait())
        uv = utr[par, i]
        for t in range(2 * DT):
            y = mm_t(uv, tqkv[layer, D + t * W:D + (t + 1) * W, :])
            kind, tt = t // DT, t % DT
            ref = vt if kind else kt
            y4 = y.reshape(CH, G, SUB, W)
            for g in range(G):
                ref[g, pl.ds(pl.multiple_of(i * CR, CR), CR), tt * W:(tt + 1) * W] = y4[:, g].reshape(CR, W).astype(BF)

    def temporal(i, layer, step):
        rows = lax.broadcasted_iota(jnp.int32, (2 * CR, WIN), 0)
        keys = lax.broadcasted_iota(jnp.int32, (2 * CR, WIN), 1)
        pos_q = i * CH + (rows & (CR - 1)) // SUB
        pos_k = (i - NC) * CH + keys // SUB
        pos = block * NC * CH + pos_q - step
        slot = jnp.where(pos < 0, pos + MF * NC * CH, pos)
        valid = pos_q - pos_k <= slot
        for h in range(HP):
            bm[h] = jnp.where(valid, bias[layer, h], -jnp.inf)

        @pl.loop(0, G // TU)
        def _(gg):
            qrows = pl.ds(pl.multiple_of(i * CR, CR), CR)
            krows = pl.ds(pl.multiple_of(i * CR, CR), WIN)
            units = [(gg * TU + d, d * 2 * CR, h) for d in range(TU) for h in range(HP)]
            for g, r, h in units:
                cols = slice(h * LANES, (h + 1) * LANES)
                sv = mm_t(stack_heads(qt[g, qrows, cols]), kt[g, krows, cols]) + bm[h]
                pb[h, r:r + 2 * CR, 0:WIN] = softmax_rows(sv)
            for g, r, h in units:
                cols = slice(h * LANES, (h + 1) * LANES)
                o2 = mm(pb[h, r:r + 2 * CR, 0:WIN], vt[g, krows, cols])
                ob[pl.ds(pl.multiple_of(g * CR, CR), CR), cols] = jnp.where(low, o2[:CR], o2[CR:]).astype(BF)

        ov = ob[...]
        for r in range(0, R, R // 2):
            for t in range(DT):
                cols = slice(t * W, (t + 1) * W)
                r0, r1 = r, r + R // 2
                g0, gn = r0 // CR, (r1 - r0) // CR
                y4 = mm(ov[r0:r1], to[:, cols]).reshape(gn, CH, SUB, W)
                for a in range(CH):
                    rows = slice(a * TK + g0 * SUB, a * TK + (g0 + gn) * SUB)
                    x[i, rows, cols] = x[i, rows, cols] + y4[:, a].reshape(gn * SUB, W)

    def mlp(i, layer, step, r0, r1):
        for a in range(r0 // TK, r1 // TK):
            def put(r, v, a=a):
                uu[a * TK + r:a * TK + r + NR, :] = v

            modulated(i, a, layer, step, 2, put)
        for t in range(FF // FT):
            for r in range(r0, r1, RH):
                hb[r:r + RH, t * FT:(t + 1) * FT] = gelu(mm(uu[r:r + RH], up[:, t * FT:(t + 1) * FT])).astype(BF)
        for r in range(r0, r1, RH):
            for t in range(DT):
                cols = slice(t * W, (t + 1) * W)
                x[i, r:r + RH, cols] = x[i, r:r + RH, cols] + mm(hb[r:r + RH], down[:, cols])

    def embed(zv):
        return tt_mm(zv.astype(BF), wi[...]).astype(BF).astype(F32)

    def ready(i, layer, step, r0=0, r1=R):
        for a in range(r0 // TK, r1 // TK):
            def put(r, v, a=a):
                ust[i, a // HS, (a % HS) * TK + r:(a % HS) * TK + r + NR, :] = v

            modulated(i, a, layer, step, 0, put)

    place = lax.broadcasted_iota(jnp.int32, (1, R), 1) // TK

    def turn(i, step):
        for q in range(0, R, NR):
            uu[q:q + NR, :] = norm(x[i, q:q + NR, :]).astype(BF)
        dt = jnp.zeros((1, R), F32)
        for a in range(CH):
            dt = jnp.where(place == a, mod[i * CH + a + (S - 1) - step, pl.ds(6 * L, 1), 0:R], dt)
        zv = z[i] + dt * mm_t(wo[...], uu[...])
        z[i] = zv
        x[i] = embed(jnp.where(first & (i * CH + place == step), nz[step], zv))

    def replace_head(step):
        i = step // CH
        zv = z[i]
        for a in range(CH):
            @pl.when(step % CH == a)
            def _(a=a):
                late[NC * CH - S + step] = zv[0:NCH, a * TK:(a + 1) * TK]

        z[i] = jnp.where(first & (i * CH + place == step), nz[step], zv)

    def begin(i):
        x[i] = embed(z[i])
        ready(i, 0, 0)
        mine = pl.ds(pl.multiple_of(core * RH, RH), RH)
        for k in range(3):
            xv = embed(zq[k, i, :, mine])
            for s in range(HS):
                gain, shift = affine(i * CH + core * HS + s, 0, 0, 0)
                us[0, i, k, s * TK:(s + 1) * TK, :] = (norm(xv[s * TK:(s + 1) * TK]) * gain + shift).astype(BF)

    @pl.loop(0, NT + 1)
    def _(m):
        n = m - 1
        layer, step, par = lax.rem(n + L, L), (n + L) // L - 1, lax.rem(n + 2, 2)
        nlayer, nstep, npar = lax.rem(m, L), m // L, lax.rem(m, 2)

        @pl.when(m > 0)
        def _():
            w_copy(0, layer).wait()
            w_copy(1, layer).wait()

            @pl.when(m == 1)
            def _():
                for q in range(L):
                    t_copy(q).wait()

            for k in (2, 3, 4):
                w_copy(k, layer).start()

            @pl.loop(0, NC + 1)
            def _(c):
                @pl.when(c == NC - 1)
                def _():
                    halo_kv(NC - 1, par, layer)

                @pl.when(c < NC)
                def _():
                    spatial(NC - 1 - c, par, n)

                @pl.when(c > 0)
                def _():
                    own_qkv(NC - c, layer)

                @pl.when(c < NC)
                def _():
                    project(NC - 1 - c, par, layer, step, n)

            for k in (2, 3, 4):
                w_copy(k, layer).wait()

            @pl.when(m < NT)
            def _():
                w_copy(0, nlayer).start()
                w_copy(1, nlayer).start()

        @pl.when(m == 0)
        def _():
            @pl.loop(0, NC)
            def _(c):
                begin(NC - 1 - c)

        def finish_step(i):
            turn(i, step)
            ready(i, nlayer, jnp.minimum(nstep, S - 1))

            @pl.when(m < NT)
            def _():
                for c in us_copies(npar, i):
                    c.start()

        @pl.when(m > 0)
        def _():
            i = NC - 1
            temporal(i, layer, step)
            for h in range(2):
                mlp(i, layer, step, h * RH, (h + 1) * RH)
                ready(i, nlayer, jnp.minimum(nstep, S - 1), h * RH, (h + 1) * RH)
                to_sib, to_a, to_b = us_copies(npar, i)

                @pl.when((layer < L - 1) & (core == h))
                def _():
                    to_a.start()

                @pl.when((layer < L - 1) & (core != h))
                def _():
                    to_b.start()
                    to_sib.start()

            @pl.when(layer == L - 1)
            def _():
                finish_step(i)

            @pl.loop(1, NC)
            def _(c):
                i = NC - 1 - c
                halo_kv(i, par, layer)
                temporal(i, layer, step)
                mlp(i, layer, step, 0, R)
                ready(i, nlayer, jnp.minimum(nstep, S - 1))

                @pl.when(layer < L - 1)
                def _():
                    for copy in us_copies(npar, i):
                        copy.start()

                @pl.when(layer == L - 1)
                def _():
                    finish_step(i)

        @pl.when((m > 0) & (layer == L - 1))
        def _():
            replace_head(step)

        @pl.when(m > 0)
        def _():
            pl.semaphore_signal(credit, inc=1, device_id=prv, device_id_type=MESH)

    pl.semaphore_wait(credit, min(2, NT))
    for k in range(NC * CH):
        zv = z[k // CH, 0:NCH, k % CH * TK:(k % CH + 1) * TK]
        if k < S:
            early[k] = zv
        else:
            late[k - S] = zv


def denoise_call(cfg, vmem, *args):
    L, S, NC, CH, TK, D, FF, HD, MT, MF, WIN = cfg
    R, HS, RH, G = CH * TK, CH // 2, CH * TK // 2, TK // SUB
    CR, SR = CH * SUB, NC * CH * SUB
    HP = D // LANES
    C = args[2].shape[0]
    KR = (NC - 1) * CR + WIN
    scr = [
        pltpu.VMEM((S - 1 + NC * CH, 6 * L + 1, D), F32),
        pltpu.VMEM((L, HP, 2 * CR, WIN), F32),
        pltpu.VMEM((NC, CPAD, R), F32),
        pltpu.VMEM((3, NC, CPAD, R), F32),
        pltpu.VMEM((S, CPAD, R), F32),
        pltpu.VMEM((CPAD, D), BF),
        pltpu.VMEM((CPAD, D), BF),
        pltpu.VMEM((NC, R, D), F32),
        pltpu.VMEM((NC, 2, RH, D), BF),
        pltpu.VMEM((2, NC, 3, RH, D), BF),
        pltpu.VMEM((HS, 4 * TK, 2 * D), BF),
        pltpu.VMEM((HS, 2 * TK, D), BF),
        pltpu.VMEM((NC, 2, RH, D), BF),
        pltpu.VMEM((NC, RH, D), BF),
        pltpu.VMEM((NC, R, D), BF),
        pltpu.VMEM((2, NC, R, D), BF),
        pltpu.VMEM((G, SR, D), BF),
        pltpu.VMEM((G, KR, D), BF),
        pltpu.VMEM((G, KR, D), BF),
        pltpu.VMEM((max(2, 2) * HP, max(4 * TK, 16 * CR), max(4 * TK, WIN)), BF),
        pltpu.VMEM((HP, 2 * CR, WIN), F32),
        pltpu.VMEM((R, D), BF),
        pltpu.VMEM((R, D), BF),
        pltpu.VMEM((R, FF), BF),
        pltpu.VMEM((3 * D, D), BF),
        pltpu.VMEM((D, D), BF),
        pltpu.VMEM((L, 3 * D, D), BF),
        pltpu.VMEM((D, D), BF),
        pltpu.VMEM((D, FF), BF),
        pltpu.VMEM((FF, D), BF),
        pltpu.SemaphoreType.DMA((NC, 3)),
        pltpu.SemaphoreType.DMA((2, NC, 3)),
        pltpu.SemaphoreType.DMA((NC,)),
        pltpu.SemaphoreType.DMA((NC,)),
        pltpu.SemaphoreType.DMA((NC,)),
        pltpu.SemaphoreType.DMA((2, NC)),
        pltpu.SemaphoreType.DMA((5 + L,)),
        pltpu.SemaphoreType.DMA((2,)),
        pltpu.SemaphoreType.DMA((3,)),
        pltpu.SemaphoreType.DMA((3,)),
        pltpu.SemaphoreType.REGULAR,
    ]
    inner = pl.BlockSpec(memory_space=pltpu.VMEM)
    outer = pl.BlockSpec(memory_space=pl.ANY)
    return pl.pallas_call(
        functools.partial(kernel, cfg),
        out_shape=(jax.ShapeDtypeStruct((NC * CH, C, TK), F32), jax.ShapeDtypeStruct((S, C, TK), F32)),
        in_specs=[pl.BlockSpec(memory_space=pltpu.SMEM)] + [inner] * 3 + [outer] * 8,
        out_specs=(inner, inner),
        scratch_shapes=scr,
        compiler_params=pltpu.CompilerParams(collective_id=0, has_side_effects=True, vmem_limit_bytes=vmem),
        name="fifo_denoise",
    )(*args)


def solution(mesh):
    MT, MF = mesh.shape["tokens"], mesh.shape["frames"]
    slot_spec = P(("videos", "frames"), "tokens", None)
    mod_spec = P(("videos", "frames"), None, None, None)
    step_spec = P(("videos", "frames"))
    noise_spec = P("videos", "tokens", None)
    emit_spec = P("videos", ("tokens", "frames"), None)
    to_sib = [(f, f ^ 1) for f in range(MF)]
    to_next_chip = [(f, (f + 2) % MF) for f in range(MF)]

    def seat(blk, q):
        here = [t for t in range(MT) if (t // 2 + blk // 2) % 2 == blk % 2 and ((t + 1) // 2) % 2 == q // 2]
        return here[0] * MF + 2 * (blk // 2) + q % 2

    places = [(blk, q) for blk in range(MF) for q in range(MT)]
    to_seat = [(q * MF + blk, seat(blk, q)) for blk, q in places]
    to_home = [(seat(blk, q), q * MF + blk) for blk, q in places]
    to_home_before = [(seat(blk, q), q * MF + (blk - 1) % MF) for blk, q in places]

    def body(z_loc, mod_loc, step_loc, noise_loc, lag_bias, w_in, w_out, w_sqkv, w_so, w_tqkv, w_to, w_up, w_down):
        SL, TK, C = z_loc.shape
        S = noise_loc.shape[0]
        L, D, FF = w_up.shape
        HD = w_so.shape[2]
        NC = CHUNKS
        CH = SL // NC
        WIN = 2 * SL * SUB
        tok, frm, chip, core, odd, half = roles(MT, MF)
        both = ("tokens", "frames")
        z_t, noise_t = jnp.swapaxes(z_loc, 1, 2), jnp.swapaxes(noise_loc, 1, 2)
        z_mine = lax.ppermute(jnp.concatenate([z_t, noise_t], axis=0), both, to_seat)

        table = jnp.concatenate([jnp.swapaxes(mod_loc, 1, 2).reshape(SL, 6 * L, D), jnp.broadcast_to(step_loc[:, None, None], (SL, 1, D))], axis=1)
        table_sib = lax.ppermute(table, "frames", to_sib)
        even_blk = jnp.where(core == 0, table, table_sib)
        odd_blk = jnp.where(core == 1, table, table_sib)
        tail = lax.ppermute(odd_blk[SL - (S - 1):], "frames", to_next_chip)
        own_tab = jnp.where(odd == 0, even_blk, odd_blk)
        prev_tab = jnp.where(odd == 0, tail, even_blk[SL - (S - 1):])

        by_output = lambda w: jnp.transpose(w, (0, 2, 3, 4, 1)).reshape(L, 3 * D, D)
        cfg = (L, S, NC, CH, TK, D, FF, HD, MT, MF, WIN)
        late, early = denoise_call(
            cfg, 67043328,
            lag_bias.reshape(L * lag_bias.shape[1], -1), z_mine, w_in, jnp.transpose(w_out), own_tab, prev_tab,
            by_output(w_sqkv), w_so.reshape(L, D, D), by_output(w_tqkv), w_to.reshape(L, D, D), w_up, w_down,
        )

        late = lax.ppermute(late, both, to_home)
        early = lax.ppermute(early, both, to_home_before)
        z_fin = jnp.swapaxes(jnp.concatenate([late[:SL - S], early], axis=0), 1, 2)
        em = jnp.moveaxis(late[SL - S:].reshape(S, C, MF, TK // MF), 2, 0)
        em = jnp.swapaxes(lax.all_to_all(em, "frames", 0, 0, tiled=True)[0], 1, 2)
        return em, z_fin

    return jax.shard_map(body, mesh=mesh, in_specs=(slot_spec, mod_spec, step_spec, noise_spec) + (P(),) * 9, out_specs=(emit_spec, slot_spec), check_vma=False)
```

```python
import functools

import jax
import jax.numpy as jnp
from jax import lax
from jax.experimental import pallas as pl
from jax.experimental.pallas import tpu as pltpu
from jax.sharding import PartitionSpec as P

MESH = pl.DeviceIdType.MESH
BF = jnp.bfloat16
F32 = jnp.float32
LANES = 128
CPAD = 16
SUB = 8
CHUNKS = 4


def mm(a, b):
    return jnp.dot(a, b, preferred_element_type=F32)


def mm_t(a, b):
    return lax.dot_general(a, b, (((1,), (1,)), ((), ())), preferred_element_type=F32)


def tt_mm(a, b):
    return lax.dot_general(a, b, (((0,), (0,)), ((), ())), preferred_element_type=F32)


def norm(xv):
    mean = jnp.mean(xv, axis=-1, keepdims=True)
    cen = xv - mean
    var = jnp.mean(cen * cen, axis=-1, keepdims=True)
    return cen * lax.rsqrt(var + 1e-6)


def gelu(hv):
    inner = 0.7978845608028654 * (hv + 0.044715 * (hv * hv * hv))
    return 0.5 * hv * (1.0 + jnp.tanh(inner))


def roles(mesh_tokens, mesh_frames):
    tok, frm = lax.axis_index("tokens"), lax.axis_index("frames")
    chip, core = frm // 2, frm % 2
    odd = (tok // 2 + chip) % 2
    half = ((tok + 1) // 2) % 2
    return tok, frm, chip, core, odd, half


def kernel(cfg, lag_bias, z_mine, w_in, w_out, own_tab, prev_tab, sqkv_h, so_h, tqkv_h, to_h, up_h, down_h, late, early,
           mod, bias, z, zq, nz, wi, wo, x, ust, us, kvs, qs, obuf, osnd, ut, utr, qt, kt, vt, pb, bm, ob, uu, hb,
           sqkv, so, tqkv, to, up, down,
           us_s, us_r, o_s, o_r, ut_s, ut_r, w_sem, t_sem, z_s, z_r, credit):
    L, S, NC, CH, TK, D, FF, HD, MT, MF, WIN = cfg
    R, HS, RH, G = CH * TK, CH // 2, CH * TK // 2, TK // SUB
    CR = CH * SUB
    SR = NC * CH * SUB
    NT = L * S
    HP = D // LANES
    W = min(256, D)
    DT = D // W
    FT = min(256, FF)
    qscale = HD ** -0.5
    NCH = w_in.shape[0]
    SU, TU, RS = min(2, HS), min(8, G), min(64, 4 * TK)

    vid = lax.axis_index("videos")
    tok, frm, chip, core, odd, _ = roles(MT, MF)
    sib_f = frm + 1 - 2 * core
    par_t = tok + 1 - 2 * (tok % 2)
    block = chip * 2 + odd
    first = block == 0
    sib = (vid, tok, sib_f)
    par_a = (vid, par_t, frm)
    par_b = (vid, par_t, sib_f)
    nxt = (vid, jnp.where(odd == 0, MT - 1 - tok, tok), jnp.where(odd == 0, frm, (frm + 2) % MF))
    prv = (vid, jnp.where(odd == 1, MT - 1 - tok, tok), jnp.where(odd == 1, frm, (frm + MF - 2) % MF))

    def w_copy(k, layer):
        src, dst = ((sqkv_h, sqkv), (so_h, so), (to_h, to), (up_h, up), (down_h, down))[k]
        return pltpu.make_async_copy(src.at[layer], dst, w_sem.at[k])

    def t_copy(layer):
        return pltpu.make_async_copy(tqkv_h.at[layer], tqkv.at[layer], w_sem.at[5 + layer])

    tables = (
        pltpu.make_async_copy(prev_tab, mod.at[0:S - 1], t_sem.at[0]),
        pltpu.make_async_copy(own_tab, mod.at[S - 1:S - 1 + NC * CH], t_sem.at[1]),
    )
    for c in tables:
        c.start()
    w_copy(0, 0).start()
    w_copy(1, 0).start()
    for layer in range(L):
        t_copy(layer).start()

    wi[...] = jnp.zeros_like(wi)
    wo[...] = jnp.zeros_like(wo)
    wi[0:NCH] = w_in[...]
    wo[0:NCH] = w_out[...]
    for ref in (z, nz):
        ref[...] = jnp.zeros_like(ref)
    for k in range(NC * CH):
        i, lanes = k // CH, slice(k % CH * TK, (k % CH + 1) * TK)
        z[i, 0:NCH, lanes] = z_mine[k]
    for k in range(S):
        for a in range(CH):
            nz[k, 0:NCH, a * TK:(a + 1) * TK] = z_mine[NC * CH + k]
    barrier = pltpu.get_barrier_semaphore()
    for dev in (sib, par_a, par_b, nxt, prv):
        pl.semaphore_signal(barrier, inc=1, device_id=dev, device_id_type=MESH)
    pl.semaphore_wait(barrier, 5)

    def remote(src, dst, ss, rs, dev):
        return pltpu.make_async_remote_copy(src_ref=src, dst_ref=dst, send_sem=ss, recv_sem=rs, device_id=dev, device_id_type=MESH)

    def us_copies(par, i):
        return (
            remote(ust.at[i, 1 - core], us.at[par, i, 0], us_s.at[i, 0], us_r.at[par, i, 0], sib),
            remote(ust.at[i, core], us.at[par, i, 1], us_s.at[i, 1], us_r.at[par, i, 1], par_a),
            remote(ust.at[i, 1 - core], us.at[par, i, 2], us_s.at[i, 2], us_r.at[par, i, 2], par_b),
        )

    def o_copy(i):
        return remote(osnd.at[i], obuf.at[i, core], o_s.at[i], o_r.at[i], sib)

    unread = TK * max(0, min(NC * CH + 1 - lag_bias.shape[1], CH - 1))

    def ut_each(par, i, act):
        def part(row):
            act(remote(ut.at[i, row:R], utr.at[par, i, row:R], ut_s.at[i], ut_r.at[par, i], nxt))

        pl.when(i == 0)(lambda: part(unread))
        pl.when(i > 0)(lambda: part(0))

    near = [remote(z, zq.at[k], z_s.at[k], z_r.at[k], dev) for k, dev in enumerate((sib, par_a, par_b))]
    for c in near:
        c.start()
    if unread:
        utr[:, 0, 0:unread, :] = jnp.zeros((2, unread, D), BF)
    for g in range(G):
        for ref in (kt, vt):
            ref[g] = jnp.zeros(ref.shape[1:], BF)

    q_row = lax.broadcasted_iota(jnp.int32, (CR, WIN), 0)
    k_col = lax.broadcasted_iota(jnp.int32, (CR, WIN), 1)
    lag = NC * CH + q_row // SUB - k_col // SUB
    lag = jnp.where((q_row & (SUB - 1)) == (k_col & (SUB - 1)), lag, -1)

    @pl.loop(0, L * HP)
    def _(lh):
        for hd in range(2):
            tile = jnp.full((CR, WIN), -jnp.inf, F32)
            for r in range(lag_bias.shape[1]):
                tile = jnp.where(lag == r, lag_bias[2 * lh + hd, r], tile)
            bias[lh // HP, lh % HP, hd * CR:(hd + 1) * CR, :] = tile

    for c in tables:
        c.wait()
    for c in near:
        c.wait()

    lane = lax.broadcasted_iota(jnp.int32, (1, LANES), 1)
    low = lane < HD

    def stack_heads(q):
        zero = jnp.zeros_like(q)
        return jnp.concatenate([jnp.where(low, q, zero), jnp.where(low, zero, q)], axis=0)

    def softmax_rows(sv):
        top = jnp.max(sv, axis=-1, keepdims=True)
        e = jnp.exp(sv - top)
        return (e * (1.0 / jnp.sum(e, axis=-1, keepdims=True))).astype(BF)

    NR = min(32, TK)

    def affine(slot, layer, step, which):
        row = slot + (S - 1) - step
        return 1.0 + mod[row, pl.ds((2 * which + 1) * L + layer, 1), :], mod[row, pl.ds(2 * which * L + layer, 1), :]

    def modulated(i, a, layer, step, which, put):
        gain, shift = affine(i * CH + a, layer, step, which)
        for r in range(0, TK, NR):
            xv = x[i, a * TK + r:a * TK + r + NR, :]
            put(r, (norm(xv) * gain + shift).astype(BF))

    def spatial(i, par, n):
        @pl.when(n > 0)
        def _():
            for c in us_copies(par, i):
                c.wait()

        own = ust[i, core]
        u_all = jnp.concatenate([own, us[par, i, 0], us[par, i, 1], us[par, i, 2]], axis=0)
        u_q = jnp.concatenate([own, us[par, i, 0]], axis=0)
        for t in range(DT):
            y = (mm_t(u_q, sqkv[t * W:(t + 1) * W, :]) * qscale).astype(BF)
            for p in range(2):
                for s in range(HS):
                    qs[s, p * TK:(p + 1) * TK, t * W:(t + 1) * W] = y[p * RH + s * TK:p * RH + (s + 1) * TK]
        for t in range(2 * DT):
            y = mm_t(u_all, sqkv[D + t * W:D + (t + 1) * W, :]).astype(BF)
            for p in range(4):
                for s in range(HS):
                    kvs[s, p * TK:(p + 1) * TK, t * W:(t + 1) * W] = y[p * RH + s * TK:p * RH + (s + 1) * TK]

        @pl.loop(0, HS // SU)
        def _(ss):
            units = [(ss * SU + d, d * HP + h, h) for d in range(SU) for h in range(HP)]
            for s, p, h in units:
                cols = slice(h * LANES, (h + 1) * LANES)
                sv = mm_t(stack_heads(qs[s, :, cols]), kvs[s, :, cols])
                for r in range(0, 4 * TK, RS):
                    pb[p, r:r + RS, 0:4 * TK] = softmax_rows(sv[r:r + RS])
            for s, p, h in units:
                cols = slice(h * LANES, (h + 1) * LANES)
                o2 = mm(pb[p, 0:4 * TK, 0:4 * TK], kvs[s, :, D + h * LANES:D + (h + 1) * LANES])
                o = jnp.where(low, o2[:2 * TK], o2[2 * TK:]).astype(BF)
                rows = pl.ds(pl.multiple_of(s * TK, TK), TK)
                obuf[i, core, rows, cols] = o[:TK]
                osnd[i, rows, cols] = o[TK:]

        o_copy(i).start()

    def project(i, par, layer, step, n):
        o_copy(i).wait()
        ov = obuf[i].reshape(R, D)
        for r in range(0, R, R // 2):
            for t in range(DT):
                cols = slice(t * W, (t + 1) * W)
                x[i, r:r + R // 2, cols] = x[i, r:r + R // 2, cols] + mm(ov[r:r + R // 2], so[:, cols])
        for a in range(CH):
            def put(r, v, a=a):
                ut[i, a * TK + r:a * TK + r + NR, :] = v

            modulated(i, a, layer, step, 1, put)

        @pl.when((i == NC - 1) & (n >= 2))
        def _():
            pl.semaphore_wait(credit, 1)

        ut_each(par, i, lambda c: c.start())

    def own_qkv(i, layer):
        uv = ut[i]
        for t in range(3 * DT):
            y = mm_t(uv, tqkv[layer, t * W:(t + 1) * W, :])
            kind, tt = t // DT, t % DT
            if kind == 0:
                y = y * qscale
            y4 = y.reshape(CH, G, SUB, W)
            for g in range(G):
                yg = y4[:, g].reshape(CR, W).astype(BF)
                if kind == 0:
                    qt[g, pl.ds(pl.multiple_of(i * CR, CR), CR), tt * W:(tt + 1) * W] = yg
                else:
                    ref = kt if kind == 1 else vt
                    ref[g, pl.ds(pl.multiple_of(SR + i * CR, CR), CR), tt * W:(tt + 1) * W] = yg

    def temporal(i, par, layer, step):
        ut_each(par, i, lambda c: c.wait())
        uv = utr[par, i]
        for t in range(2 * DT):
            y = mm_t(uv, tqkv[layer, D + t * W:D + (t + 1) * W, :])
            kind, tt = t // DT, t % DT
            ref = vt if kind else kt
            y4 = y.reshape(CH, G, SUB, W)
            for g in range(G):
                ref[g, pl.ds(pl.multiple_of(i * CR, CR), CR), tt * W:(tt + 1) * W] = y4[:, g].reshape(CR, W).astype(BF)
        rows = lax.broadcasted_iota(jnp.int32, (2 * CR, WIN), 0)
        keys = lax.broadcasted_iota(jnp.int32, (2 * CR, WIN), 1)
        pos_q = i * CH + (rows & (CR - 1)) // SUB
        pos_k = (i - NC) * CH + keys // SUB
        pos = block * NC * CH + pos_q - step
        slot = jnp.where(pos < 0, pos + MF * NC * CH, pos)
        valid = pos_q - pos_k <= slot
        for h in range(HP):
            bm[h] = jnp.where(valid, bias[layer, h], -jnp.inf)

        @pl.loop(0, G // TU)
        def _(gg):
            qrows = pl.ds(pl.multiple_of(i * CR, CR), CR)
            krows = pl.ds(pl.multiple_of(i * CR, CR), WIN)
            units = [(gg * TU + d, d * 2 * CR, h) for d in range(TU) for h in range(HP)]
            for g, r, h in units:
                cols = slice(h * LANES, (h + 1) * LANES)
                sv = mm_t(stack_heads(qt[g, qrows, cols]), kt[g, krows, cols]) + bm[h]
                pb[h, r:r + 2 * CR, 0:WIN] = softmax_rows(sv)
            for g, r, h in units:
                cols = slice(h * LANES, (h + 1) * LANES)
                o2 = mm(pb[h, r:r + 2 * CR, 0:WIN], vt[g, krows, cols])
                ob[pl.ds(pl.multiple_of(g * CR, CR), CR), cols] = jnp.where(low, o2[:CR], o2[CR:]).astype(BF)

        ov = ob[...]
        for r in range(0, R, R // 2):
            for t in range(DT):
                cols = slice(t * W, (t + 1) * W)
                r0, r1 = r, r + R // 2
                g0, gn = r0 // CR, (r1 - r0) // CR
                y4 = mm(ov[r0:r1], to[:, cols]).reshape(gn, CH, SUB, W)
                for a in range(CH):
                    rows = slice(a * TK + g0 * SUB, a * TK + (g0 + gn) * SUB)
                    x[i, rows, cols] = x[i, rows, cols] + y4[:, a].reshape(gn * SUB, W)

    def mlp(i, layer, step):
        for a in range(CH):
            def put(r, v, a=a):
                uu[a * TK + r:a * TK + r + NR, :] = v

            modulated(i, a, layer, step, 2, put)
        for t in range(FF // FT):
            for r in range(0, R, RH):
                hb[r:r + RH, t * FT:(t + 1) * FT] = gelu(mm(uu[r:r + RH], up[:, t * FT:(t + 1) * FT])).astype(BF)
        for r in range(0, R, R // 2):
            for t in range(DT):
                cols = slice(t * W, (t + 1) * W)
                x[i, r:r + R // 2, cols] = x[i, r:r + R // 2, cols] + mm(hb[r:r + R // 2], down[:, cols])

    def embed(zv):
        return tt_mm(zv.astype(BF), wi[...]).astype(BF).astype(F32)

    def ready(i, layer, step):
        for a in range(CH):
            def put(r, v, a=a):
                ust[i, a // HS, (a % HS) * TK + r:(a % HS) * TK + r + NR, :] = v

            modulated(i, a, layer, step, 0, put)

    place = lax.broadcasted_iota(jnp.int32, (1, R), 1) // TK

    def turn(i, step):
        for q in range(0, R, NR):
            uu[q:q + NR, :] = norm(x[i, q:q + NR, :]).astype(BF)
        dt = jnp.zeros((1, R), F32)
        for a in range(CH):
            dt = jnp.where(place == a, mod[i * CH + a + (S - 1) - step, pl.ds(6 * L, 1), 0:R], dt)
        zv = z[i] + dt * mm_t(wo[...], uu[...])
        z[i] = zv
        x[i] = embed(jnp.where(first & (i * CH + place == step), nz[step], zv))

    def replace_head(step):
        i = step // CH
        zv = z[i]
        for a in range(CH):
            @pl.when(step % CH == a)
            def _(a=a):
                late[NC * CH - S + step] = zv[0:NCH, a * TK:(a + 1) * TK]

        z[i] = jnp.where(first & (i * CH + place == step), nz[step], zv)

    def begin(i):
        x[i] = embed(z[i])
        ready(i, 0, 0)
        mine = pl.ds(pl.multiple_of(core * RH, RH), RH)
        for k in range(3):
            xv = embed(zq[k, i, :, mine])
            for s in range(HS):
                gain, shift = affine(i * CH + core * HS + s, 0, 0, 0)
                us[0, i, k, s * TK:(s + 1) * TK, :] = (norm(xv[s * TK:(s + 1) * TK]) * gain + shift).astype(BF)

    @pl.loop(0, NT + 1)
    def _(m):
        n = m - 1
        layer, step, par = lax.rem(n + L, L), (n + L) // L - 1, lax.rem(n + 2, 2)
        nlayer, nstep, npar = lax.rem(m, L), m // L, lax.rem(m, 2)

        @pl.when(m > 0)
        def _():
            w_copy(0, layer).wait()
            w_copy(1, layer).wait()

            @pl.when(m == 1)
            def _():
                for q in range(L):
                    t_copy(q).wait()

            for k in (2, 3, 4):
                w_copy(k, layer).start()

            @pl.loop(0, NC + 1)
            def _(c):
                @pl.when(c < NC)
                def _():
                    spatial(NC - 1 - c, par, n)

                @pl.when(c > 0)
                def _():
                    own_qkv(NC - c, layer)

                @pl.when(c < NC)
                def _():
                    project(NC - 1 - c, par, layer, step, n)

            for k in (2, 3, 4):
                w_copy(k, layer).wait()

            @pl.when(m < NT)
            def _():
                w_copy(0, nlayer).start()
                w_copy(1, nlayer).start()

        @pl.loop(0, NC)
        def _(c):
            i = NC - 1 - c

            @pl.when(m == 0)
            def _():
                begin(i)

            @pl.when(m > 0)
            def _():
                temporal(i, par, layer, step)
                mlp(i, layer, step)
                ready(i, nlayer, jnp.minimum(nstep, S - 1))

                @pl.when(layer == L - 1)
                def _():
                    turn(i, step)
                    ready(i, nlayer, jnp.minimum(nstep, S - 1))

                @pl.when(m < NT)
                def _():
                    for c in us_copies(npar, i):
                        c.start()

        @pl.when((m > 0) & (layer == L - 1))
        def _():
            replace_head(step)

        @pl.when(m > 0)
        def _():
            pl.semaphore_signal(credit, inc=1, device_id=prv, device_id_type=MESH)

    pl.semaphore_wait(credit, min(2, NT))
    for k in range(NC * CH):
        zv = z[k // CH, 0:NCH, k % CH * TK:(k % CH + 1) * TK]
        if k < S:
            early[k] = zv
        else:
            late[k - S] = zv


def denoise_call(cfg, vmem, *args):
    L, S, NC, CH, TK, D, FF, HD, MT, MF, WIN = cfg
    R, HS, RH, G = CH * TK, CH // 2, CH * TK // 2, TK // SUB
    CR, SR = CH * SUB, NC * CH * SUB
    HP = D // LANES
    C = args[2].shape[0]
    KR = (NC - 1) * CR + WIN
    scr = [
        pltpu.VMEM((S - 1 + NC * CH, 6 * L + 1, D), F32),
        pltpu.VMEM((L, HP, 2 * CR, WIN), F32),
        pltpu.VMEM((NC, CPAD, R), F32),
        pltpu.VMEM((3, NC, CPAD, R), F32),
        pltpu.VMEM((S, CPAD, R), F32),
        pltpu.VMEM((CPAD, D), BF),
        pltpu.VMEM((CPAD, D), BF),
        pltpu.VMEM((NC, R, D), F32),
        pltpu.VMEM((NC, 2, RH, D), BF),
        pltpu.VMEM((2, NC, 3, RH, D), BF),
        pltpu.VMEM((HS, 4 * TK, 2 * D), BF),
        pltpu.VMEM((HS, 2 * TK, D), BF),
        pltpu.VMEM((NC, 2, RH, D), BF),
        pltpu.VMEM((NC, RH, D), BF),
        pltpu.VMEM((NC, R, D), BF),
        pltpu.VMEM((2, NC, R, D), BF),
        pltpu.VMEM((G, SR, D), BF),
        pltpu.VMEM((G, KR, D), BF),
        pltpu.VMEM((G, KR, D), BF),
        pltpu.VMEM((max(2, 2) * HP, max(4 * TK, 16 * CR), max(4 * TK, WIN)), BF),
        pltpu.VMEM((HP, 2 * CR, WIN), F32),
        pltpu.VMEM((R, D), BF),
        pltpu.VMEM((R, D), BF),
        pltpu.VMEM((R, FF), BF),
        pltpu.VMEM((3 * D, D), BF),
        pltpu.VMEM((D, D), BF),
        pltpu.VMEM((L, 3 * D, D), BF),
        pltpu.VMEM((D, D), BF),
        pltpu.VMEM((D, FF), BF),
        pltpu.VMEM((FF, D), BF),
        pltpu.SemaphoreType.DMA((NC, 3)),
        pltpu.SemaphoreType.DMA((2, NC, 3)),
        pltpu.SemaphoreType.DMA((NC,)),
        pltpu.SemaphoreType.DMA((NC,)),
        pltpu.SemaphoreType.DMA((NC,)),
        pltpu.SemaphoreType.DMA((2, NC)),
        pltpu.SemaphoreType.DMA((5 + L,)),
        pltpu.SemaphoreType.DMA((2,)),
        pltpu.SemaphoreType.DMA((3,)),
        pltpu.SemaphoreType.DMA((3,)),
        pltpu.SemaphoreType.REGULAR,
    ]
    inner = pl.BlockSpec(memory_space=pltpu.VMEM)
    outer = pl.BlockSpec(memory_space=pl.ANY)
    return pl.pallas_call(
        functools.partial(kernel, cfg),
        out_shape=(jax.ShapeDtypeStruct((NC * CH, C, TK), F32), jax.ShapeDtypeStruct((S, C, TK), F32)),
        in_specs=[pl.BlockSpec(memory_space=pltpu.SMEM)] + [inner] * 3 + [outer] * 8,
        out_specs=(inner, inner),
        scratch_shapes=scr,
        compiler_params=pltpu.CompilerParams(collective_id=0, has_side_effects=True, vmem_limit_bytes=vmem),
        name="fifo_denoise",
    )(*args)


def solution(mesh):
    MT, MF = mesh.shape["tokens"], mesh.shape["frames"]
    slot_spec = P(("videos", "frames"), "tokens", None)
    mod_spec = P(("videos", "frames"), None, None, None)
    step_spec = P(("videos", "frames"))
    noise_spec = P("videos", "tokens", None)
    emit_spec = P("videos", ("tokens", "frames"), None)
    to_sib = [(f, f ^ 1) for f in range(MF)]
    to_next_chip = [(f, (f + 2) % MF) for f in range(MF)]

    def seat(blk, q):
        here = [t for t in range(MT) if (t // 2 + blk // 2) % 2 == blk % 2 and ((t + 1) // 2) % 2 == q // 2]
        return here[0] * MF + 2 * (blk // 2) + q % 2

    places = [(blk, q) for blk in range(MF) for q in range(MT)]
    to_seat = [(q * MF + blk, seat(blk, q)) for blk, q in places]
    to_home = [(seat(blk, q), q * MF + blk) for blk, q in places]
    to_home_before = [(seat(blk, q), q * MF + (blk - 1) % MF) for blk, q in places]

    def body(z_loc, mod_loc, step_loc, noise_loc, lag_bias, w_in, w_out, w_sqkv, w_so, w_tqkv, w_to, w_up, w_down):
        SL, TK, C = z_loc.shape
        S = noise_loc.shape[0]
        L, D, FF = w_up.shape
        HD = w_so.shape[2]
        NC = CHUNKS
        CH = SL // NC
        WIN = 2 * SL * SUB
        tok, frm, chip, core, odd, half = roles(MT, MF)
        both = ("tokens", "frames")
        z_t, noise_t = jnp.swapaxes(z_loc, 1, 2), jnp.swapaxes(noise_loc, 1, 2)
        z_mine = lax.ppermute(jnp.concatenate([z_t, noise_t], axis=0), both, to_seat)

        table = jnp.concatenate([jnp.swapaxes(mod_loc, 1, 2).reshape(SL, 6 * L, D), jnp.broadcast_to(step_loc[:, None, None], (SL, 1, D))], axis=1)
        table_sib = lax.ppermute(table, "frames", to_sib)
        even_blk = jnp.where(core == 0, table, table_sib)
        odd_blk = jnp.where(core == 1, table, table_sib)
        tail = lax.ppermute(odd_blk[SL - (S - 1):], "frames", to_next_chip)
        own_tab = jnp.where(odd == 0, even_blk, odd_blk)
        prev_tab = jnp.where(odd == 0, tail, even_blk[SL - (S - 1):])

        by_output = lambda w: jnp.transpose(w, (0, 2, 3, 4, 1)).reshape(L, 3 * D, D)
        cfg = (L, S, NC, CH, TK, D, FF, HD, MT, MF, WIN)
        late, early = denoise_call(
            cfg, 67043328,
            lag_bias.reshape(L * lag_bias.shape[1], -1), z_mine, w_in, jnp.transpose(w_out), own_tab, prev_tab,
            by_output(w_sqkv), w_so.reshape(L, D, D), by_output(w_tqkv), w_to.reshape(L, D, D), w_up, w_down,
        )

        late = lax.ppermute(late, both, to_home)
        early = lax.ppermute(early, both, to_home_before)
        z_fin = jnp.swapaxes(jnp.concatenate([late[:SL - S], early], axis=0), 1, 2)
        em = jnp.moveaxis(late[SL - S:].reshape(S, C, MF, TK // MF), 2, 0)
        em = jnp.swapaxes(lax.all_to_all(em, "frames", 0, 0, tiled=True)[0], 1, 2)
        return em, z_fin

    return jax.shard_map(body, mesh=mesh, in_specs=(slot_spec, mod_spec, step_spec, noise_spec) + (P(),) * 9, out_specs=(emit_spec, slot_spec), check_vma=False)
```
